256 devices in a mesh: seq: 32 (over x, y, core), tensor: 8 (over z).
Axes of the slice: x: 4, y: 4, z: 8, core: 2. Of those that a mesh axis runs over, the one named last changes fastest.
Arguments:
- queries: bfloat16 [32768, 8, 128], P('seq', 'tensor'), may hold values from -16 to 16
- keys: bfloat16 [32768, 128], P('seq'), may hold values from -6 to 6
- values: bfloat16 [32768, 128], P('seq'), may hold values from -6 to 6
- doc_ids: int32 [32768], P('seq'), may hold values from 0 to 31, never falling along the last dimension, each value on 1 to 4096 neighbouring positions
- w_query: bfloat16 [8, 128, 64], P('tensor'), may hold values from -0.5 to 0.5
- w_key: bfloat16 [128, 64], replicated, may hold values from -0.5 to 0.5
Outputs:
- student: bfloat16 [32768, 8, 128], P('seq', 'tensor')
- grad_wq: float32 [8, 128, 64], P('tensor')
- grad_key_weight: float32 [128, 64], replicated
- key_feature_grads: float32 [32768, 128], P('seq', 'tensor')
The draws below stay inside these ranges and needn't reach their ends.
Inputs may be any that keep to these rules, and one draw needn't show every extreme that they name: `doc_ids`: document numbers never fall along the sequence and each number is used; each document has 1 to 4096 positions, and one has exactly 4096.
All inputs are finite; a program needn't handle non-finite values.
Results may differ from the reference program's by a relative error of at most 0.017.
Values may be sent and summed in bfloat16 or wider, within the bound.
A program may use at most 64 MiB of HBM per device.

```python
import math
import jax
import jax.numpy as jnp
import numpy as np
from jax import lax

HEAD_SIZE = 128
HEADS = 8
FEAT = 128
REACH = 4
TOK_DEV = 1024
HALF = 64
SEQ = 32768
MOST = 4096
N_SEQ = 32


def paired_draw(key):
    folded = jax.random.fold_in(key, 4099)
    first_key, second_key = jax.random.split(folded, 2)
    key_draw = jnp.clip(jax.random.normal(first_key, (SEQ, HEAD_SIZE), jnp.float32), -6.0, 6.0)
    query_draw = jnp.clip(jax.random.normal(second_key, (SEQ, HEADS, HEAD_SIZE), jnp.float32), -6.0, 6.0)
    return (query_draw, key_draw)


def draw_queries(key, part):
    return paired_draw(key)[0].astype(jnp.bfloat16)


def draw_keys(key, part):
    return paired_draw(key)[1].astype(jnp.bfloat16)


def shard_levels(rng, dims, shards, low, high):
    def one(axis_at, blocks):
        heights = jax.random.uniform(jax.random.fold_in(jax.random.fold_in(rng, 6), axis_at), (blocks,), jnp.float32, low / len(shards), high / len(shards))
        return jnp.repeat(jnp.exp(heights), dims[axis_at] // blocks).reshape((-1,) + (1,) * (len(dims) - axis_at - 1))

    loudness = one(*shards[0])
    for cut in shards[1:]:
        loudness = loudness * one(*cut)
    return loudness


def profile(count, total, most, skew):
    portions = [(1 << 20) // math.isqrt(grade ** skew) + 1 for grade in range(2, count + 1)]
    spare, holding = total - most - (count - 1), [1] * (count - 1)
    while spare > 0:
        candidates = [i for i in range(count - 1) if holding[i] < most]
        whole, remaining = sum([portions[i] for i in candidates]), spare
        for i in candidates:
            addition = min(most - holding[i], max(1, remaining * portions[i] // whole), spare)
            holding[i] = holding[i] + addition
            spare = spare - addition
    return np.array([most] + holding)


def uneven_parts(rng, count, total, bound, slope):
    if count == 2:
        one = jax.random.randint(rng, (), max(1, total - bound), min(bound, total - 1) + 1)
        return jnp.stack([one, total - one])
    sizes = jnp.asarray(profile(count, total, bound, slope), jnp.int32)
    twos = (count - 1) // 2
    source_of, taker = sizes[1:1 + 2 * twos:2], sizes[2:2 + 2 * twos:2]
    slack = jnp.minimum(source_of - 1, bound - taker)
    moved = jax.random.randint(jax.random.fold_in(rng, 1), (twos,), 0, 1 << 20) % (slack + 1)
    sizes = sizes.at[1:1 + 2 * twos:2].set(source_of - moved).at[2:2 + 2 * twos:2].set(taker + moved)
    return sizes[jax.random.permutation(jax.random.fold_in(rng, 2), count)]


def bell_draw(own_key, extent, spread, reach, cuts=(), held_as=jnp.bfloat16):
    array = jax.random.normal(own_key, extent, jnp.float32) * spread
    if len(cuts) > 0:
        array = shard_levels(own_key, extent, cuts, -0.22, 0.18) * array
    return jnp.clip(array, min=-reach, max=reach).astype(held_as)


def setup_inputs(seed: int = 0) -> dict:
    arg_keys = jax.random.split(jax.random.key(seed), 7)
    queries = draw_queries(jax.random.fold_in(arg_keys[6], 71), 0)
    keys = draw_keys(jax.random.fold_in(arg_keys[6], 71), 0)
    values = bell_draw(arg_keys[2], (SEQ, HEAD_SIZE), 1.0, 6.0, ((0, 32),))
    doc_ids = jnp.searchsorted(jnp.cumsum(uneven_parts(arg_keys[3], N_SEQ, SEQ, MOST, 2)), jnp.arange(SEQ), side="right").astype(jnp.int32)
    w_query = bell_draw(arg_keys[4], (HEADS, HEAD_SIZE, HALF), HEAD_SIZE ** -0.5, 0.5, ((0, 8),))
    w_key = bell_draw(arg_keys[5], (HEAD_SIZE, HALF), HEAD_SIZE ** -0.5, 0.5)
    return dict(queries=queries, keys=keys, values=values, doc_ids=doc_ids, w_query=w_query, w_key=w_key)


NEGATIVE = -1e30
exact_setting = lax.Precision.HIGHEST


def feature(logits):
    return jnp.concatenate([jax.nn.softmax(logits, axis=-1), jax.nn.softmax(-logits, axis=-1)], axis=-1)


def feature_back(features, incoming_grad):
    middle = features.shape[-1] // 2
    upper_half = features[..., :middle]
    lower_half = features[..., middle:]
    grad_upper = incoming_grad[..., :middle]
    grad_lower = incoming_grad[..., middle:]
    upper_term = upper_half * (grad_upper - jnp.sum(grad_upper * upper_half, axis=-1, keepdims=True))
    lower_term = lower_half * (grad_lower - jnp.sum(grad_lower * lower_half, axis=-1, keepdims=True))
    return upper_term - lower_term


def join_states(earlier, later):
    earlier_state, earlier_sum, earlier_code = earlier
    later_state, later_sum, later_code = later
    vacant = later_code == 0.0
    matching = (later_code == earlier_code).astype(jnp.float32)
    joined_state = jnp.where(vacant, earlier_state, later_state + matching * earlier_state)
    joined_sum = jnp.where(vacant, earlier_sum, later_sum + matching * earlier_sum)
    return joined_state, joined_sum, jnp.where(vacant, earlier_code, later_code)


def to_bfloat(array_in):
    return lax.optimization_barrier(array_in.astype(jnp.bfloat16)).astype(jnp.float32)


def chain_step(carry, element):
    return join_states(carry, element), carry


def reference(queries, keys, values, doc_ids, w_query, w_key):
    count_of_rows = TOK_DEV
    pad_rows = REACH * count_of_rows
    score_scale = HEAD_SIZE ** -0.5
    doc_codes = (doc_ids + 1).astype(jnp.int32)
    key_features = feature(jnp.dot(keys, w_key, preferred_element_type=jnp.float32))
    key_feat_b = to_bfloat(key_features)
    keys_wide = jnp.concatenate([jnp.zeros((pad_rows, HEAD_SIZE), jnp.float32), keys.astype(jnp.float32)], axis=0)
    values_wide = jnp.concatenate([jnp.zeros((pad_rows, HEAD_SIZE), jnp.float32), values.astype(jnp.float32)], axis=0)
    codes_wide = jnp.concatenate([jnp.zeros((pad_rows,), jnp.int32), doc_codes], axis=0)
    key_blocks = key_feat_b.reshape(N_SEQ, count_of_rows, FEAT)
    blocked_values = values.astype(jnp.float32).reshape(N_SEQ, count_of_rows, HEAD_SIZE)
    code_blocks = doc_codes.reshape(N_SEQ, count_of_rows)
    query_blocks = queries.astype(jnp.float32).reshape(N_SEQ, count_of_rows, HEADS, HEAD_SIZE)
    w_query_f = w_query.astype(jnp.float32)

    def local_state(feature_rows, value_rows, code_rows):
        chosen = (code_rows == code_rows[-1]).astype(jnp.float32)[:, None] * feature_rows
        return (jnp.einsum('kf,kd->fd', chosen, value_rows, precision=exact_setting), jnp.sum(chosen, axis=0), code_rows[-1].astype(jnp.float32))

    identity = (jnp.zeros((FEAT, HEAD_SIZE), jnp.float32), jnp.zeros((FEAT,), jnp.float32), jnp.zeros((), jnp.float32))
    local_states = jax.vmap(local_state)(key_blocks, blocked_values, code_blocks)
    _, incoming = lax.scan(chain_step, identity, local_states)
    query_pos = jnp.arange(count_of_rows, dtype=jnp.int32)
    key_pos = jnp.arange(pad_rows + count_of_rows, dtype=jnp.int32) - pad_rows

    def block_terms(inputs):
        block_index, query_rows, carried_state, carried_sum, carried_code = inputs
        first_row = (block_index * count_of_rows).astype(jnp.int32)
        code_rows = lax.dynamic_slice_in_dim(doc_codes, first_row, count_of_rows)
        window_keys = lax.dynamic_slice_in_dim(keys_wide, first_row, pad_rows + count_of_rows)
        window_values = lax.dynamic_slice_in_dim(values_wide, first_row, pad_rows + count_of_rows)
        window_codes = lax.dynamic_slice_in_dim(codes_wide, first_row, pad_rows + count_of_rows)
        scores = jnp.einsum('qhd,kd->qhk', query_rows, window_keys, precision=exact_setting) * score_scale
        allowed = (code_rows[:, None] == window_codes[None, :]) & (key_pos[None, :] <= query_pos[:, None])
        row_top = jnp.max(jnp.where(allowed[:, None, :], scores, NEGATIVE), axis=-1, keepdims=True)
        weights = jnp.where(allowed[:, None, :], jnp.exp(scores - row_top), 0.0)
        teacher = jnp.einsum('qhk,kd->qhd', to_bfloat(weights), window_values, precision=exact_setting) / jnp.sum(weights, axis=-1)[..., None]
        feature_rows = lax.dynamic_index_in_dim(key_blocks, block_index, 0, keepdims=False)
        value_rows = lax.dynamic_index_in_dim(blocked_values, block_index, 0, keepdims=False)
        query_features = feature(jnp.einsum('qhd,hdf->qhf', query_rows, w_query_f, precision=exact_setting))
        query_feat_b = to_bfloat(query_features)
        local_mask = (code_rows[:, None] == code_rows[None, :]) & (query_pos[None, :] <= query_pos[:, None])
        products = jnp.where(local_mask[:, None, :], jnp.einsum('qhf,kf->qhk', query_feat_b, feature_rows, precision=exact_setting), 0.0)
        receive = (code_rows.astype(jnp.float32) == carried_code).astype(jnp.float32)
        numerator = jnp.einsum('qhk,kd->qhd', to_bfloat(products), value_rows, precision=exact_setting) + receive[:, None, None] * jnp.einsum('qhf,fd->qhd', query_feat_b, carried_state, precision=exact_setting)
        denominator = jnp.sum(products, axis=-1) + receive[:, None] * jnp.einsum('qhf,f->qh', query_feat_b, carried_sum, precision=exact_setting)
        estimate = numerator / denominator[..., None]
        grad_out = (2.0 / SEQ) * (estimate - teacher)
        grad_num = grad_out / denominator[..., None]
        grad_den = -jnp.sum(grad_out * estimate, axis=-1) / denominator
        grad_prod = to_bfloat(jnp.where(local_mask[:, None, :], jnp.einsum('qhd,kd->qhk', to_bfloat(grad_num), value_rows, precision=exact_setting) + grad_den[..., None], 0.0))
        grad_qf = jnp.einsum('qhk,kf->qhf', grad_prod, feature_rows, precision=exact_setting) + receive[:, None, None] * (jnp.einsum('qhd,fd->qhf', grad_num, carried_state, precision=exact_setting) + grad_den[..., None] * carried_sum)
        grad_kf_local = jnp.einsum('qhk,qhf->kf', grad_prod, query_feat_b, precision=exact_setting)
        leading = (code_rows == code_rows[0]).astype(jnp.float32)[:, None, None] * query_feat_b
        adjoint_state = jnp.einsum('qhf,qhd->fd', leading, grad_num, precision=exact_setting)
        adjoint_sum = jnp.einsum('qhf,qh->f', leading, grad_den, precision=exact_setting)
        grad_aq = to_bfloat(feature_back(query_features, grad_qf))
        grad_wq_block = jnp.einsum('qhd,qhf->hdf', query_rows, grad_aq, precision=exact_setting)
        return estimate.astype(jnp.bfloat16), grad_kf_local, adjoint_state, adjoint_sum, code_rows[0].astype(jnp.float32), grad_wq_block

    block_ids = jnp.arange(N_SEQ, dtype=jnp.int32)
    students, grad_kf_local, adjoint_states, adjoint_sums, leading_codes, grad_wq_blocks = lax.map(block_terms, (block_ids, query_blocks, incoming[0], incoming[1], incoming[2]))
    _, adjoint_entering = lax.scan(chain_step, identity, (adjoint_states, adjoint_sums, leading_codes), reverse=True)
    receive_back = (code_blocks.astype(jnp.float32) == adjoint_entering[2][:, None]).astype(jnp.float32)
    additional_terms = jnp.einsum('woa,wxa->wox', blocked_values, adjoint_entering[0], precision=exact_setting) + adjoint_entering[1][:, None, :]
    grad_kf = grad_kf_local + receive_back[:, :, None] * additional_terms
    grad_attention_key = to_bfloat(feature_back(key_features.reshape(N_SEQ, count_of_rows, FEAT), grad_kf))
    grad_key_weight = jnp.einsum('srg,srv->gv', keys.astype(jnp.float32).reshape(N_SEQ, count_of_rows, HEAD_SIZE), grad_attention_key, precision=exact_setting)
    grad_wq = jnp.sum(grad_wq_blocks, axis=0)
    key_feature_grads = grad_kf.reshape(SEQ, FEAT) * float(SEQ)
    return students.reshape(SEQ, HEADS, HEAD_SIZE), grad_wq, grad_key_weight, key_feature_grads
```

```python
import functools

import jax
import jax.numpy as jnp
from jax import lax
from jax.experimental import pallas as pl
from jax.experimental.pallas import tpu as pltpu
from jax.sharding import PartitionSpec as P

F32 = jnp.float32
BF16 = jnp.bfloat16
MESH = pl.DeviceIdType.MESH
VMEM = pltpu.VMEM

REACH = 4
SIDE = 4
NEGATIVE = -1e30
LOG2E = 1.4426950408889634
OWN_TILE = 256
FAR_TILE = 512
ADJ_ROWS = 144


def dot(a, b, ca, cb):
    return lax.dot_general(a, b, (((ca,), (cb,)), ((), ())), preferred_element_type=F32)


def remote(src, dst, send_sem, recv_sem, **where):
    return pltpu.make_async_remote_copy(
        src_ref=src,
        dst_ref=dst,
        send_sem=send_sem,
        recv_sem=recv_sem,
        device_id=where,
        device_id_type=MESH,
    )


def signal(sem, **where):
    pl.semaphore_signal(sem, inc=1, device_id=where, device_id_type=MESH)


def window_kernel(
    n_seq,
    n_z,
    k_ref,
    v_ref,
    c_ref,
    wk_ref,
    wv_ref,
    wc_ref,
    code_send,
    code_recv,
    slice_send,
    slice_recv,
    own_send,
    ring_send,
    ring_recv,
    pair_send,
    pair_recv,
):
    s = lax.axis_index("seq")
    z = lax.axis_index("tensor")
    core = lax.rem(s, 2)
    partner = s + 1 - 2 * core
    part = k_ref.shape[0] // n_z

    def later(d):
        return lax.rem(s + d, n_seq)

    def turn(d):
        return lax.rem(z + d + n_z, n_z)

    def rows(p):
        return pl.ds(pl.multiple_of(p * part, part), part)

    barrier = pltpu.get_barrier_semaphore()
    for d in range(1, REACH + 1):
        signal(barrier, seq=later(n_seq - d))
    signal(barrier, seq=partner)
    signal(barrier, tensor=turn(1))
    signal(barrier, tensor=turn(-1))
    pl.semaphore_wait(barrier, REACH + 3)

    pairs = ((k_ref, wk_ref), (v_ref, wv_ref))
    started = []
    for target, (distance, slot) in enumerate(((4 - core, 3 - core), (3 - core, 2 - core))):
        for kv, (own, window) in enumerate(pairs):
            copy = remote(
                own.at[rows(z)],
                window.at[slot, rows(z)],
                slice_send.at[target, kv],
                slice_recv.at[core, kv],
                seq=later(distance),
            )
            copy.start()
            started.append(copy)
    for d in range(1, REACH + 1):
        copy = remote(
            c_ref, wc_ref.at[d - 1], code_send.at[d - 1], code_recv.at[d - 1], seq=later(d)
        )
        copy.start()
        started.append(copy)

    @pl.when(core == 0)
    def _():
        for kv, (own, window) in enumerate(pairs):
            remote(own, window.at[0], own_send.at[kv], pair_recv.at[kv], seq=partner).start()

    slots = (3 - core, 2 - core)

    def pass_to_partner(i, kv, piece):
        window = pairs[kv][1]

        def send(slot):
            remote(
                window.at[slots[i], rows(piece)],
                window.at[slot, rows(piece)],
                pair_send.at[i, kv],
                pair_recv.at[kv],
                seq=partner,
            ).start()

        if i == 1:
            send(3 - 3 * core)
        else:

            @pl.when(core == 1)
            def _():
                send(1)

    def ring_copy(way, step, i, kv):
        window = pairs[kv][1]
        piece = turn(1 - step) if way == 0 else turn(step - 1)
        return remote(
            window.at[slots[i], rows(piece)],
            window.at[slots[i], rows(piece)],
            ring_send.at[way, step - 1, i, kv],
            ring_recv.at[way, step - 1, i, kv],
            tensor=turn(1 if way == 0 else -1),
        )

    last = n_z // 2

    def active(way, step, i):
        return step < last or (step == last and way == i)

    for i in range(2):
        for kv in range(2):
            window = pairs[kv][1]
            here = window.at[slots[i], rows(z)]
            remote(
                here, here, slice_send.at[0, kv], slice_recv.at[i, kv], seq=partner
            ).wait_recv()
            for way in range(2):
                copy = ring_copy(way, 1, i, kv)
                copy.start()
                started.append(copy)
            pass_to_partner(i, kv, z)
    for step in range(1, last + 1):
        for i in range(2):
            for kv in range(2):
                for way in range(2):
                    if not active(way, step, i):
                        continue
                    window = pairs[kv][1]
                    piece = turn(-step) if way == 0 else turn(step)
                    here = window.at[slots[i], rows(piece)]
                    remote(
                        here,
                        here,
                        ring_send.at[way, step - 1, i, kv],
                        ring_recv.at[way, step - 1, i, kv],
                        tensor=turn(1 if way == 0 else -1),
                    ).wait_recv()
                    if active(way, step + 1, i):
                        copy = ring_copy(way, step + 1, i, kv)
                        copy.start()
                        started.append(copy)
                    pass_to_partner(i, kv, piece)

    for copy in started:
        copy.wait_send()
    for d in range(1, REACH + 1):
        remote(
            c_ref, wc_ref.at[d - 1], code_send.at[d - 1], code_recv.at[d - 1], seq=later(d)
        ).wait_recv()
    for kv, (own, window) in enumerate(pairs):
        both = window.at[pl.ds(0, 2)]
        remote(both, both, own_send.at[kv], pair_recv.at[kv], seq=partner).wait_recv()
        whole = window.at[0]
        remote(whole, whole, pair_send.at[1, kv], pair_recv.at[kv], seq=partner).wait_send()

        @pl.when(core == 1)
        def _():
            remote(whole, whole, pair_send.at[0, kv], pair_recv.at[kv], seq=partner).wait_send()

        @pl.when(core == 0)
        def _():
            remote(own, whole, own_send.at[kv], pair_recv.at[kv], seq=partner).wait_send()


def whole(n):
    return [pl.BlockSpec(memory_space=VMEM)] * n


def window_of(keys, values, codes, n_seq, n_z):
    block = (REACH, *keys.shape)
    dma = pltpu.SemaphoreType.DMA
    return pl.pallas_call(
        functools.partial(window_kernel, n_seq, n_z),
        out_shape=(
            jax.ShapeDtypeStruct(block, keys.dtype),
            jax.ShapeDtypeStruct(block, values.dtype),
            jax.ShapeDtypeStruct((REACH, *codes.shape), codes.dtype),
        ),
        in_specs=whole(3),
        out_specs=tuple(whole(3)),
        scratch_shapes=[
            dma((REACH,)),
            dma((REACH,)),
            dma((2, 2)),
            dma((2, 2)),
            dma((2,)),
            dma((2, n_z // 2, 2, 2)),
            dma((2, n_z // 2, 2, 2)),
            dma((2, 2)),
            dma((2,)),
        ],
        compiler_params=pltpu.CompilerParams(collective_id=0, has_side_effects=True),
        name="window",
    )(keys, values, codes)


def features(rows, weights_t):
    logits = dot(weights_t, rows, 1, 1)
    up = jnp.exp(logits - jnp.max(logits, axis=0, keepdims=True))
    down = jnp.exp(jnp.min(logits, axis=0, keepdims=True) - logits)
    up = up / jnp.sum(up, axis=0, keepdims=True)
    down = down / jnp.sum(down, axis=0, keepdims=True)
    return jnp.concatenate([up, down], axis=0)


def features_back(feat, grad):
    half = feat.shape[0] // 2
    p, m, a, b = feat[:half], feat[half:], grad[:half], grad[half:]
    upper = p * (a - jnp.sum(a * p, axis=0, keepdims=True))
    lower = m * (b - jnp.sum(b * m, axis=0, keepdims=True))
    return upper - lower


def transposed(x):
    return x.astype(F32).T.astype(x.dtype)


def lane_copies(row, count):
    return jnp.broadcast_to(row, (count, row.shape[1])).T


def across(column, width):
    return jnp.concatenate([column] * (width // column.shape[1]), axis=1)


def attend_kernel(
    grad_scale,
    q_ref,
    k_ref,
    v_ref,
    c_ref,
    wk_ref,
    wv_ref,
    wc_ref,
    wq_ref,
    wkey_ref,
    student_ref,
    gkf_ref,
    adj_ref,
    gwq_ref,
    kf_ref,
    kcol_ref,
    fcol_ref,
    vt_ref,
    fvt_ref,
    kfb_ref,
    top_ref,
    sum_ref,
    acc_ref,
    num_ref,
    den_ref,
    state_ref,
    ssum_ref,
    qf_ref,
    gqf_ref,
):
    count, width = q_ref.shape
    factor = width**-0.5 * LOG2E
    code = c_ref[...].astype(F32)
    leading = code[:, :1]
    lead = (code == leading).astype(F32)

    wkey_t = transposed(wkey_ref[...])
    kf = features(k_ref[...], wkey_t)
    kf_ref[...] = kf
    kft = kf.astype(BF16)
    kfb_ref[...] = kf.T.astype(BF16)
    qf = features(q_ref[...], transposed(wq_ref[0]))
    qf_ref[...] = qf
    qft = qf.astype(BF16)
    vt_ref[...] = transposed(v_ref[...])
    kcol_ref[...] = lane_copies(code, width)

    def own_mask(start, size, limit):
        same = across(kcol_ref[:limit], size) == code[:, start : start + size]
        key_at = lax.broadcasted_iota(jnp.int32, (limit, size), 0)
        query_at = lax.broadcasted_iota(jnp.int32, (limit, size), 1) + start
        return same & (key_at <= query_at)

    for start in range(0, count, OWN_TILE):
        limit = start + OWN_TILE
        cols = slice(start, limit)
        mask = own_mask(start, OWN_TILE, limit)
        scores = dot(k_ref[:limit], q_ref[cols], 1, 1)
        scores = jnp.where(mask, scores * factor, NEGATIVE)
        top = jnp.max(scores, axis=0, keepdims=True)
        weights = jnp.exp2(scores - top)
        top_ref[:, cols] = top
        sum_ref[:, cols] = jnp.sum(weights, axis=0, keepdims=True)
        acc_ref[:, cols] = dot(vt_ref[:, :limit], weights.astype(BF16), 1, 0)
        products = jnp.where(mask, dot(kfb_ref[:limit], qft[:, cols], 1, 0), 0.0)
        den_ref[:, cols] = jnp.sum(products, axis=0, keepdims=True)
        num_ref[:, cols] = dot(vt_ref[:, :limit], products.astype(BF16), 1, 0)

    state_ref[...] = jnp.zeros_like(state_ref)
    ssum_ref[...] = jnp.zeros_like(ssum_ref)

    def far_block(d, carry):
        far_code = wc_ref[d].astype(F32)
        shared = (far_code == leading).astype(F32)

        @pl.when(jnp.max(shared) > 0.0)
        def _():
            fcol_ref[...] = lane_copies(far_code, width)
            fvt_ref[...] = transposed(wv_ref[d])
            chosen = features(wk_ref[d], wkey_t).astype(BF16).astype(F32) * shared
            state_ref[...] += dot(chosen.astype(BF16), wv_ref[d], 1, 0)
            ssum_ref[...] += jnp.broadcast_to(
                jnp.sum(chosen, axis=1, keepdims=True), ssum_ref.shape
            )
            for first in range(0, count, FAR_TILE):
                cols = slice(first, first + FAR_TILE)
                for at in range(0, count, FAR_TILE):
                    keys = slice(at, at + FAR_TILE)
                    met = (far_code[:, keys] == code[:, first : first + 1]).astype(F32)

                    @pl.when(jnp.max(met) > 0.0)
                    def _(cols=cols, keys=keys):
                        mask = across(fcol_ref[keys], FAR_TILE) == code[:, cols]
                        scores = dot(wk_ref[d, keys], q_ref[cols], 1, 1)
                        scores = jnp.where(mask, scores * factor, NEGATIVE)
                        old = top_ref[:, cols]
                        top = jnp.maximum(old, jnp.max(scores, axis=0, keepdims=True))
                        weights = jnp.exp2(scores - top)
                        shrink = jnp.exp2(old - top)
                        top_ref[:, cols] = top
                        sum_ref[:, cols] = sum_ref[:, cols] * shrink + jnp.sum(
                            weights, axis=0, keepdims=True
                        )
                        acc_ref[:, cols] = acc_ref[:, cols] * shrink + dot(
                            fvt_ref[:, keys], weights.astype(BF16), 1, 0
                        )

        return carry

    lax.fori_loop(0, REACH, far_block, 0)

    state = state_ref[...]
    state_b = state.astype(BF16)
    state_sum = ssum_ref[:, :1]
    teacher = acc_ref[...] / sum_ref[...]
    numerator = num_ref[...] + lead * dot(state.T.astype(BF16), qft, 1, 0)
    denominator = den_ref[...] + lead * jnp.sum(
        qft.astype(F32) * state_sum, axis=0, keepdims=True
    )
    estimate = numerator / denominator
    student_ref[...] = estimate.T.astype(BF16).reshape(student_ref.shape)
    grad_out = grad_scale * (estimate - teacher)
    grad_num = grad_out / denominator
    grad_den = -jnp.sum(grad_out * estimate, axis=0, keepdims=True) / denominator
    gnt = grad_num.astype(BF16)

    extra = ADJ_ROWS - width
    row = lax.broadcasted_iota(jnp.int32, (extra, count), 0)
    tail = jnp.where(row == 0, grad_den * lead, 0.0)
    masked = jnp.concatenate([grad_num * lead, tail], axis=0).astype(BF16)
    adjoint = dot(masked, qft, 1, 1)
    mark = lax.broadcasted_iota(jnp.int32, adjoint.shape, 0)
    adj_ref[...] = jnp.where(mark == width + 1, leading, adjoint).astype(BF16)

    gqf_ref[...] = lead * (dot(state_b, gnt, 1, 0) + state_sum * grad_den)
    for start in range(0, count, OWN_TILE):
        limit = start + OWN_TILE
        cols = slice(start, limit)
        mask = own_mask(start, OWN_TILE, limit)
        grad_prod = dot(v_ref[:limit], gnt[:, cols], 1, 0) + grad_den[:, cols]
        grad_prod = jnp.where(mask, grad_prod, 0.0).astype(BF16)
        gqf_ref[:, cols] += dot(kft[:, :limit], grad_prod, 1, 0)
        part = dot(qft[:, cols], grad_prod, 1, 1)
        if start:
            gkf_ref[:, :start] += part[:, :start]
        gkf_ref[:, cols] = part[:, start:]
    grad_aq = features_back(qf_ref[...], gqf_ref[...]).astype(BF16)
    gwq_ref[...] = dot(grad_aq, q_ref[...], 1, 0)


def attend(queries, keys, values, codes, wk, wv, wc, w_query, w_key, grad_scale):
    count, width = keys.shape
    half = w_key.shape[1]
    feat = 2 * half
    return pl.pallas_call(
        functools.partial(attend_kernel, grad_scale),
        out_shape=(
            jax.ShapeDtypeStruct((count, width), BF16),
            jax.ShapeDtypeStruct((feat, count), F32),
            jax.ShapeDtypeStruct((ADJ_ROWS, feat), BF16),
            jax.ShapeDtypeStruct((half, width), F32),
            jax.ShapeDtypeStruct((feat, count), F32),
        ),
        in_specs=whole(9),
        out_specs=tuple(whole(5)),
        scratch_shapes=[
            VMEM((count, width), F32),
            VMEM((count, width), F32),
            VMEM((width, count), BF16),
            VMEM((width, count), BF16),
            VMEM((count, feat), BF16),
            VMEM((1, count), F32),
            VMEM((1, count), F32),
            VMEM((width, count), F32),
            VMEM((width, count), F32),
            VMEM((1, count), F32),
            VMEM((feat, width), F32),
            VMEM((feat, width), F32),
            VMEM((feat, count), F32),
            VMEM((feat, count), F32),
        ],
        name="attend",
    )(queries, keys, values, codes, wk, wv, wc, w_query, w_key)


def finish_kernel(
    n_seq,
    n_z,
    total,
    adj_ref,
    gkf_ref,
    kf_ref,
    k_ref,
    v_ref,
    c_ref,
    gwq_ref,
    gwq_out,
    gwk_out,
    kfg_out,
    adj_in,
    spread_ref,
    gather_ref,
    core_ref,
    y_ref,
    x_ref,
    z_ref,
    adj_send,
    adj_recv,
    spread_send,
    spread_recv,
    core_send,
    core_recv,
    y_send,
    y_recv,
    x_send,
    x_recv,
    z_send,
    z_recv,
):
    s = lax.axis_index("seq")
    z = lax.axis_index("tensor")
    core = lax.rem(s, 2)
    partner = s + 1 - 2 * core
    y = lax.rem(s // 2, SIDE)
    x = s // (2 * SIDE)
    count, width = k_ref.shape
    half = gwq_ref.shape[0]
    share = kf_ref.shape[0] // n_z

    def along_y(i):
        return lax.rem(y + i, SIDE)

    def along_x(i):
        return lax.rem(x + i, SIDE)

    def along_z(i):
        return lax.rem(z + i, n_z)

    def seq_of(at_x, at_y):
        return (at_x * SIDE + at_y) * 2 + core

    barrier = pltpu.get_barrier_semaphore()
    for d in range(1, REACH + 1):
        signal(barrier, seq=lax.rem(s + d, n_seq))
    signal(barrier, seq=partner)
    for i in range(1, SIDE):
        signal(barrier, seq=seq_of(x, along_y(i)))
        signal(barrier, seq=seq_of(along_x(i), y))
    for i in range(1, n_z):
        signal(barrier, tensor=along_z(i))
    pl.semaphore_wait(barrier, REACH + 1 + 2 * (SIDE - 1) + n_z - 1)

    started = []

    def send(*args, **where):
        copy = remote(*args, **where)
        copy.start()
        started.append(copy)

    for d in range(1, REACH + 1):
        send(
            adj_ref,
            adj_in.at[d - 1],
            adj_send.at[d - 1],
            adj_recv.at[d - 1],
            seq=lax.rem(s + n_seq - d, n_seq),
        )
    code = c_ref[...].astype(F32)
    final = code[:, count - 1 :]
    vt = v_ref[...].astype(F32).T
    one = lax.broadcasted_iota(jnp.int32, (ADJ_ROWS - width, count), 0) == 0
    vt = jnp.concatenate([vt, one.astype(F32)], axis=0).astype(BF16)
    back = (code == final).astype(F32)

    entering = jnp.zeros(adj_ref.shape, F32)
    for d in range(1, REACH + 1):
        here = adj_in.at[d - 1]
        remote(here, here, adj_send.at[d - 1], adj_recv.at[d - 1], seq=partner).wait_recv()
        arrived = adj_in[d - 1].astype(F32)
        entering = entering + jnp.where(arrived[width + 1 : width + 2] == final, arrived, 0.0)
    added = dot(transposed(entering.astype(BF16)), vt, 1, 0)
    grad_kf = gkf_ref[...] + back * added
    spread_ref[...] = (grad_kf * total).astype(BF16)
    for i in range(1, n_z):
        to = along_z(i)
        send(
            spread_ref.at[pl.ds(pl.multiple_of(to * share, share), share)],
            gather_ref.at[z],
            spread_send.at[i - 1],
            spread_recv.at[z],
            tensor=to,
        )
    gather_ref[z] = spread_ref[pl.ds(pl.multiple_of(z * share, share), share)]

    grad_ak = features_back(kf_ref[...], grad_kf).astype(BF16)
    grad_wk = dot(grad_ak, k_ref[...], 1, 0)
    core_ref[core] = jnp.concatenate([gwq_ref[...], grad_wk], axis=0).astype(BF16)

    def wait(ref, at, send_sems, recv_sems):
        here = ref.at[at]
        remote(here, here, send_sems.at[0], recv_sems.at[at], seq=partner).wait_recv()

    def summed(ref):
        result = ref[0].astype(F32)
        for i in range(1, ref.shape[0]):
            result = result + ref[i].astype(F32)
        return result

    send(core_ref.at[core], core_ref.at[core], core_send.at[0], core_recv.at[core], seq=partner)
    wait(core_ref, 1 - core, core_send, core_recv)
    y_ref[y] = summed(core_ref).astype(BF16)
    for i in range(1, SIDE):
        to = seq_of(x, along_y(i))
        send(y_ref.at[y], y_ref.at[y], y_send.at[i - 1], y_recv.at[y], seq=to)
    for i in range(1, SIDE):
        wait(y_ref, along_y(i), y_send, y_recv)
    x_ref[x] = summed(y_ref).astype(BF16)
    for i in range(1, SIDE):
        to = seq_of(along_x(i), y)
        send(x_ref.at[x], x_ref.at[x], x_send.at[i - 1], x_recv.at[x], seq=to)
    for i in range(1, SIDE):
        wait(x_ref, along_x(i), x_send, x_recv)
    over_seq = summed(x_ref)
    z_ref[z] = over_seq[half:].astype(BF16)
    for i in range(1, n_z):
        send(z_ref.at[z], z_ref.at[z], z_send.at[i - 1], z_recv.at[z], tensor=along_z(i))
    gwq_out[...] = over_seq[:half].T.reshape(gwq_out.shape)
    for i in range(1, n_z):
        wait(gather_ref, along_z(i), spread_send, spread_recv)
    kfg_out[...] = summed(gather_ref).T
    for i in range(1, n_z):
        wait(z_ref, along_z(i), z_send, z_recv)
    gwk_out[...] = summed(z_ref).T
    for copy in started:
        copy.wait_send()


def finish(adjoint, grad_kf, key_feat, keys, values, codes, gwq, n_seq, n_z, total):
    count, width = keys.shape
    feat = key_feat.shape[0]
    half = feat // 2
    dma = pltpu.SemaphoreType.DMA
    return pl.pallas_call(
        functools.partial(finish_kernel, n_seq, n_z, total),
        out_shape=(
            jax.ShapeDtypeStruct((1, width, half), F32),
            jax.ShapeDtypeStruct((width, half), F32),
            jax.ShapeDtypeStruct((count, feat // n_z), F32),
        ),
        in_specs=whole(7),
        out_specs=tuple(whole(3)),
        scratch_shapes=[
            VMEM((REACH, ADJ_ROWS, feat), BF16),
            VMEM((feat, count), BF16),
            VMEM((n_z, feat // n_z, count), BF16),
            VMEM((2, feat, width), BF16),
            VMEM((SIDE, feat, width), BF16),
            VMEM((SIDE, feat, width), BF16),
            VMEM((n_z, half, width), BF16),
            dma((REACH,)),
            dma((REACH,)),
            dma((n_z - 1,)),
            dma((n_z,)),
            dma((1,)),
            dma((2,)),
            dma((SIDE - 1,)),
            dma((SIDE,)),
            dma((SIDE - 1,)),
            dma((SIDE,)),
            dma((n_z - 1,)),
            dma((n_z,)),
        ],
        compiler_params=pltpu.CompilerParams(collective_id=1, has_side_effects=True),
        name="finish",
    )(adjoint, grad_kf, key_feat, keys, values, codes, gwq)


def solution(mesh):
    n_seq, n_z = mesh.shape["seq"], mesh.shape["tensor"]

    def shards(queries, keys, values, doc_ids, w_query, w_key):
        count, width = keys.shape
        codes = (doc_ids + 1).reshape(1, count)
        wk, wv, wc = window_of(keys, values, codes, n_seq, n_z)
        student, grad_kf, adjoint, gwq, key_feat = attend(
            queries.reshape(count, width),
            keys,
            values,
            codes,
            wk,
            wv,
            wc,
            w_query,
            w_key,
            2.0 / (count * n_seq),
        )
        grad_wq, grad_wk, key_feature_grads = finish(
            adjoint, grad_kf, key_feat, keys, values, codes, gwq, n_seq, n_z, float(count * n_seq)
        )
        return student.reshape(queries.shape), grad_wq, grad_wk, key_feature_grads

    return jax.shard_map(
        shards,
        mesh=mesh,
        in_specs=(
            P("seq", "tensor", None),
            P("seq", None),
            P("seq", None),
            P("seq"),
            P("tensor", None, None),
            P(),
        ),
        out_specs=(P("seq", "tensor", None), P("tensor", None, None), P(), P("seq", "tensor")),
        check_vma=False,
    )
```

```python
import functools

import jax
import jax.numpy as jnp
from jax import lax
from jax.experimental import pallas as pl
from jax.experimental.pallas import tpu as pltpu
from jax.sharding import PartitionSpec as P

F32 = jnp.float32
BF16 = jnp.bfloat16
MESH = pl.DeviceIdType.MESH
VMEM = pltpu.VMEM

REACH = 4
SIDE = 4
NEGATIVE = -1e30
LOG2E = 1.4426950408889634
TILE = 256
ADJ_ROWS = 144


def dot(a, b, ca, cb):
    return lax.dot_general(a, b, (((ca,), (cb,)), ((), ())), preferred_element_type=F32)


def remote(src, dst, send_sem, recv_sem, **where):
    return pltpu.make_async_remote_copy(
        src_ref=src,
        dst_ref=dst,
        send_sem=send_sem,
        recv_sem=recv_sem,
        device_id=where,
        device_id_type=MESH,
    )


def signal(sem, **where):
    pl.semaphore_signal(sem, inc=1, device_id=where, device_id_type=MESH)


def features(rows, weights_t):
    logits = dot(weights_t, rows, 1, 1)
    up = jnp.exp(logits - jnp.max(logits, axis=0, keepdims=True))
    down = jnp.exp(jnp.min(logits, axis=0, keepdims=True) - logits)
    up = up / jnp.sum(up, axis=0, keepdims=True)
    down = down / jnp.sum(down, axis=0, keepdims=True)
    return jnp.concatenate([up, down], axis=0)


def features_back(feat, grad):
    half = feat.shape[0] // 2
    p, m, a, b = feat[:half], feat[half:], grad[:half], grad[half:]
    upper = p * (a - jnp.sum(a * p, axis=0, keepdims=True))
    lower = m * (b - jnp.sum(b * m, axis=0, keepdims=True))
    return upper - lower


def transposed(x):
    return x.astype(F32).T.astype(x.dtype)


def lane_copies(row, count):
    return jnp.broadcast_to(row, (count, row.shape[1])).T


def across(column, width):
    return jnp.concatenate([column] * (width // column.shape[1]), axis=1)


def fused_kernel(
    n_seq,
    n_z,
    q_ref,
    k_ref,
    v_ref,
    c_ref,
    wq_ref,
    wkey_ref,
    student_ref,
    gwq_out,
    gwk_out,
    kfg_out,
    wk_ref,
    wv_ref,
    wc_ref,
    kcol_ref,
    fcol_ref,
    vt_ref,
    kfb_ref,
    kf_ref,
    qf_ref,
    top_ref,
    sum_ref,
    den_ref,
    acc_ref,
    num_ref,
    state_ref,
    ssum_ref,
    gqf_ref,
    gkf_ref,
    adj_ref,
    adj_in,
    spread_ref,
    gather_ref,
    core_ref,
    y_ref,
    x_ref,
    z_ref,
    code_send,
    code_recv,
    slice_send,
    slice_recv,
    own_send,
    own_recv,
    ring_send,
    ring_recv,
    pair_send,
    pair_recv,
    adj_send,
    adj_recv,
    spread_send,
    spread_recv,
    core_send,
    core_recv,
    y_send,
    y_recv,
    x_send,
    x_recv,
    z_send,
    z_recv,
):
    count, width = k_ref.shape
    half = wkey_ref.shape[0]
    total = float(count * n_seq)
    grad_scale = 2.0 / total
    factor = width**-0.5 * LOG2E
    s = lax.axis_index("seq")
    z = lax.axis_index("tensor")
    core = lax.rem(s, 2)
    partner = s + 1 - 2 * core
    y = lax.rem(s // 2, SIDE)
    x = s // (2 * SIDE)
    part = count // n_z
    share = 2 * half // n_z

    def later(d):
        return lax.rem(s + d, n_seq)

    def turn(d):
        return lax.rem(z + d + n_z, n_z)

    def along_y(i):
        return lax.rem(y + i, SIDE)

    def along_x(i):
        return lax.rem(x + i, SIDE)

    def seq_of(at_x, at_y):
        return (at_x * SIDE + at_y) * 2 + core

    def rows(p):
        return pl.ds(pl.multiple_of(p * part, part), part)

    barrier = pltpu.get_barrier_semaphore()
    for d in range(1, REACH + 1):
        signal(barrier, seq=later(n_seq - d))
        signal(barrier, seq=later(d))
    signal(barrier, seq=partner)
    for i in range(1, SIDE):
        signal(barrier, seq=seq_of(x, along_y(i)))
        signal(barrier, seq=seq_of(along_x(i), y))
    for i in range(1, n_z):
        signal(barrier, tensor=turn(i))
    pl.semaphore_wait(barrier, 2 * REACH + 1 + 2 * (SIDE - 1) + n_z - 1)

    started = []

    def send(*args, **where):
        copy = remote(*args, **where)
        copy.start()
        started.append(copy)

    def arrive(here, send_sem, recv_sem):
        remote(here, here, send_sem, recv_sem, seq=partner).wait_recv()

    pairs = ((k_ref, wk_ref), (v_ref, wv_ref))
    for target, (distance, slot) in enumerate(((4 - core, 3 - core), (3 - core, 2 - core))):
        for kv, (own, window) in enumerate(pairs):
            send(
                own.at[rows(z)],
                window.at[slot, rows(z)],
                slice_send.at[target, kv],
                slice_recv.at[core, kv],
                seq=later(distance),
            )
    for d in range(1, REACH + 1):
        send(c_ref, wc_ref.at[d - 1], code_send.at[d - 1], code_recv.at[d - 1], seq=later(d))

    @pl.when(core == 0)
    def _():
        for kv, (own, window) in enumerate(pairs):
            remote(own, window.at[0], own_send.at[kv], own_recv.at[kv], seq=partner).start()

    slots = (3 - core, 2 - core)

    def pass_to_partner(i, kv, piece, order):
        window = pairs[kv][1]

        def go(slot):
            remote(
                window.at[slots[i], rows(piece)],
                window.at[slot, rows(piece)],
                pair_send.at[i, kv],
                pair_recv.at[i, kv, order],
                seq=partner,
            ).start()

        if i == 1:
            go(3 - 3 * core)
        else:

            @pl.when(core == 1)
            def _():
                go(1)

    def from_partner(order, piece):
        for kv in range(2):
            here = pairs[kv][1].at[0, rows(piece)]
            arrive(here, pair_send.at[1, kv], pair_recv.at[1, kv, order])

            @pl.when(core == 0)
            def _():
                arrive(here, pair_send.at[0, kv], pair_recv.at[0, kv, order])

    last = n_z // 2

    def active(way, step, i):
        return step < last or (step == last and way == i)

    def ring_copy(way, step, i, kv):
        here = pairs[kv][1].at[slots[i], rows(turn(1 - step) if way == 0 else turn(step - 1))]
        send(
            here,
            here,
            ring_send.at[way, step - 1, i, kv],
            ring_recv.at[way, step - 1, i, kv],
            tensor=turn(1 if way == 0 else -1),
        )

    def ring_step(step):
        for i in range(2):
            for kv in range(2):
                for way in range(2):
                    if not active(way, step, i):
                        continue
                    piece = turn(-step) if way == 0 else turn(step)
                    here = pairs[kv][1].at[slots[i], rows(piece)]
                    arrive(here, ring_send.at[way, step - 1, i, kv], ring_recv.at[way, step - 1, i, kv])
                    if active(way, step + 1, i):
                        ring_copy(way, step + 1, i, kv)
                    pass_to_partner(i, kv, piece, 2 * step - 1 if step == last else 2 * step - 1 + way)

    code = c_ref[...].astype(F32)
    leading = code[:, :1]
    lead = (code == leading).astype(F32)
    wkey_t = wkey_ref[...]
    kf = features(k_ref[...], wkey_t)
    kf_ref[...] = kf
    kft = kf.astype(BF16)
    kfb_ref[...] = kf.T.astype(BF16)
    qf = features(q_ref[...], wq_ref[...])
    qf_ref[...] = qf
    qft = qf.astype(BF16)
    vt_ref[:width] = transposed(v_ref[...])
    one = lax.broadcasted_iota(jnp.int32, (ADJ_ROWS - width, count), 0) == 0
    vt_ref[width:] = one.astype(F32).astype(BF16)
    kcol_ref[...] = lane_copies(code, width)

    def own_mask(start, limit):
        same = across(kcol_ref[:limit], TILE) == code[:, start:limit]
        key_at = lax.broadcasted_iota(jnp.int32, (limit, TILE), 0)
        query_at = lax.broadcasted_iota(jnp.int32, (limit, TILE), 1) + start
        return same & (key_at <= query_at)

    def own_tile(start):
        limit = start + TILE
        cols = slice(start, limit)
        mask = own_mask(start, limit)
        scores = dot(k_ref[:limit], q_ref[cols], 1, 1)
        scores = jnp.where(mask, scores * factor, NEGATIVE)
        top = jnp.max(scores, axis=0, keepdims=True)
        weights = jnp.exp2(scores - top)
        top_ref[:, cols] = top
        sum_ref[:, cols] = jnp.sum(weights, axis=0, keepdims=True)
        acc_ref[:, cols] = dot(vt_ref[:width, :limit], weights.astype(BF16), 1, 0)
        products = jnp.where(mask, dot(kfb_ref[:limit], qft[:, cols], 1, 0), 0.0)
        den_ref[:, cols] = jnp.sum(products, axis=0, keepdims=True)
        num_ref[:, cols] = dot(vt_ref[:width, :limit], products.astype(BF16), 1, 0)

    def far_pieces(pieces):
        places = [(d, rows(p), p) for d in range(REACH) for p in pieces]
        keys = jnp.concatenate([wk_ref[d, r] for d, r, _ in places], axis=0)
        vals = jnp.concatenate([wv_ref[d, r] for d, r, _ in places], axis=0)
        column = jnp.concatenate([fcol_ref[d, r] for d, r, _ in places], axis=0)
        shared = jnp.concatenate([wc_ref[d, :, rows(p)] for d, _, p in places], axis=1)
        shared = (shared.astype(F32) == leading).astype(F32)
        chosen = features(keys, wkey_t).astype(BF16).astype(F32) * shared
        state_ref[...] += dot(chosen.astype(BF16), vals, 1, 0)
        ssum_ref[...] += jnp.broadcast_to(jnp.sum(chosen, axis=1, keepdims=True), ssum_ref.shape)
        vals_t = transposed(vals)
        for start in range(0, count, TILE):
            cols = slice(start, start + TILE)
            mask = across(column, TILE) == code[:, cols]
            scores = dot(keys, q_ref[cols], 1, 1)
            scores = jnp.where(mask, scores * factor, NEGATIVE)
            old = top_ref[:, cols]
            top = jnp.maximum(old, jnp.max(scores, axis=0, keepdims=True))
            weights = jnp.exp2(scores - top)
            shrink = jnp.exp2(old - top)
            top_ref[:, cols] = top
            sum_ref[:, cols] = sum_ref[:, cols] * shrink + jnp.sum(weights, axis=0, keepdims=True)
            acc_ref[:, cols] = acc_ref[:, cols] * shrink + dot(vals_t, weights.astype(BF16), 1, 0)

    for start in range(0, count // 2, TILE):
        own_tile(start)
    for d in range(REACH):
        arrive(wc_ref.at[d], code_send.at[d], code_recv.at[d])
        fcol_ref[d] = lane_copies(wc_ref[d].astype(F32), width)
    state_ref[...] = jnp.zeros_like(state_ref)
    ssum_ref[...] = jnp.zeros_like(ssum_ref)
    for i in range(2):
        for kv in range(2):
            here = pairs[kv][1].at[slots[i], rows(z)]
            arrive(here, slice_send.at[0, kv], slice_recv.at[i, kv])
            for way in range(2):
                ring_copy(way, 1, i, kv)
            pass_to_partner(i, kv, z, 0)
    for start in range(count // 2, count, TILE):
        own_tile(start)

    @pl.when(core == 1)
    def _():
        for kv in range(2):
            arrive(pairs[kv][1].at[0], own_send.at[kv], own_recv.at[kv])

    ring_step(1)
    from_partner(0, z)
    far_pieces((z,))
    for step in range(1, last - 1):
        ring_step(step + 1)
        for way in range(2):
            from_partner(2 * step - 1 + way, turn(-step) if way == 0 else turn(step))
        far_pieces((turn(-step), turn(step)))
    step = last - 1
    for way in range(2):
        from_partner(2 * step - 1 + way, turn(-step) if way == 0 else turn(step))
    far_pieces((turn(-step), turn(step)))
    ring_step(last)
    from_partner(2 * last - 1, turn(last))
    far_pieces((turn(last),))

    state = state_ref[...]
    state_sum = ssum_ref[:, :1]
    teacher = acc_ref[...] / sum_ref[...]
    numerator = num_ref[...] + lead * dot(state.T.astype(BF16), qft, 1, 0)
    denominator = den_ref[...] + lead * jnp.sum(
        qft.astype(F32) * state_sum, axis=0, keepdims=True
    )
    estimate = numerator / denominator
    grad_out = grad_scale * (estimate - teacher)
    grad_num = grad_out / denominator
    grad_den = -jnp.sum(grad_out * estimate, axis=0, keepdims=True) / denominator
    gnt = grad_num.astype(BF16)

    row = lax.broadcasted_iota(jnp.int32, (ADJ_ROWS - width, count), 0)
    tail = jnp.where(row == 0, grad_den * lead, 0.0)
    masked = jnp.concatenate([grad_num * lead, tail], axis=0).astype(BF16)
    adjoint = dot(masked, qft, 1, 1)
    mark = lax.broadcasted_iota(jnp.int32, adjoint.shape, 0)
    adj_ref[...] = jnp.where(mark == width + 1, leading, adjoint).astype(BF16)
    for d in range(1, REACH + 1):
        send(
            adj_ref,
            adj_in.at[d - 1],
            adj_send.at[d - 1],
            adj_recv.at[d - 1],
            seq=later(n_seq - d),
        )

    gqf_ref[...] = lead * (dot(state.astype(BF16), gnt, 1, 0) + state_sum * grad_den)
    for start in range(0, count, TILE):
        limit = start + TILE
        cols = slice(start, limit)
        grad_prod = dot(v_ref[:limit], gnt[:, cols], 1, 0) + grad_den[:, cols]
        grad_prod = jnp.where(own_mask(start, limit), grad_prod, 0.0).astype(BF16)
        gqf_ref[:, cols] += dot(kft[:, :limit], grad_prod, 1, 0)
        piece = dot(qft[:, cols], grad_prod, 1, 1)
        if start:
            gkf_ref[:, :start] += piece[:, :start]
        gkf_ref[:, cols] = piece[:, start:]

    def wait(ref, which, at, send_sems, recv_sems):
        here = ref.at[which, at]
        arrive(here, send_sems.at[which, 0], recv_sems.at[which, at])

    def summed(ref, which):
        result = ref[which, 0].astype(F32)
        for i in range(1, ref.shape[1]):
            result = result + ref[which, i].astype(F32)
        return result

    def over_core(which, value):
        core_ref[which, core] = value.astype(BF16)
        here = core_ref.at[which, core]
        send(here, here, core_send.at[which, 0], core_recv.at[which, core], seq=partner)

    def over_y(which):
        wait(core_ref, which, 1 - core, core_send, core_recv)
        y_ref[which, y] = summed(core_ref, which).astype(BF16)
        here = y_ref.at[which, y]
        for i in range(1, SIDE):
            to = seq_of(x, along_y(i))
            send(here, here, y_send.at[which, i - 1], y_recv.at[which, y], seq=to)

    def over_x(which):
        for i in range(1, SIDE):
            wait(y_ref, which, along_y(i), y_send, y_recv)
        x_ref[which, x] = summed(y_ref, which).astype(BF16)
        here = x_ref.at[which, x]
        for i in range(1, SIDE):
            to = seq_of(along_x(i), y)
            send(here, here, x_send.at[which, i - 1], x_recv.at[which, x], seq=to)

    def over_seq(which):
        for i in range(1, SIDE):
            wait(x_ref, which, along_x(i), x_send, x_recv)
        return summed(x_ref, which)

    grad_aq = features_back(qf_ref[...], gqf_ref[...]).astype(BF16)
    over_core(0, dot(grad_aq, q_ref[...], 1, 0))
    student_ref[...] = estimate.T.astype(BF16)
    over_y(0)

    final = code[:, count - 1 :]
    back = (code == final).astype(F32)
    entering = jnp.zeros(adj_ref.shape, F32)
    for d in range(REACH):
        arrive(adj_in.at[d], adj_send.at[d], adj_recv.at[d])
        arrived = adj_in[d].astype(F32)
        entering = entering + jnp.where(arrived[width + 1 : width + 2] == final, arrived, 0.0)
    added = dot(entering.T.astype(BF16), vt_ref[...], 1, 0)
    grad_kf = gkf_ref[...] + back * added
    spread_ref[...] = (grad_kf * total).astype(BF16)
    for i in range(1, n_z):
        to = turn(i)
        send(
            spread_ref.at[pl.ds(pl.multiple_of(to * share, share), share)],
            gather_ref.at[0, z],
            spread_send.at[0, i - 1],
            spread_recv.at[0, z],
            tensor=to,
        )
    gather_ref[0, z] = spread_ref[pl.ds(pl.multiple_of(z * share, share), share)]

    grad_ak = features_back(kf_ref[...], grad_kf).astype(BF16)
    over_core(1, dot(grad_ak, k_ref[...], 1, 0))
    over_x(0)
    over_y(1)
    gwq_out[...] = over_seq(0)
    over_x(1)
    z_ref[0, z] = over_seq(1).astype(BF16)
    here = z_ref.at[0, z]
    for i in range(1, n_z):
        send(here, here, z_send.at[0, i - 1], z_recv.at[0, z], tensor=turn(i))
    for i in range(1, n_z):
        wait(gather_ref, 0, turn(i), spread_send, spread_recv)
    kfg_out[...] = summed(gather_ref, 0)
    for i in range(1, n_z):
        wait(z_ref, 0, turn(i), z_send, z_recv)
    gwk_out[...] = summed(z_ref, 0)

    for copy in started:
        copy.wait_send()
    for kv, (own, window) in enumerate(pairs):
        block = window.at[0]
        remote(block, block, pair_send.at[1, kv], own_recv.at[kv], seq=partner).wait_send()

        @pl.when(core == 1)
        def _():
            remote(block, block, pair_send.at[0, kv], own_recv.at[kv], seq=partner).wait_send()

        @pl.when(core == 0)
        def _():
            remote(own, block, own_send.at[kv], own_recv.at[kv], seq=partner).wait_send()


def fused(queries, keys, values, codes, wq_t, wkey_t, n_seq, n_z):
    count, width = keys.shape
    half = wkey_t.shape[0]
    feat = 2 * half
    dma = pltpu.SemaphoreType.DMA
    return pl.pallas_call(
        functools.partial(fused_kernel, n_seq, n_z),
        out_shape=(
            jax.ShapeDtypeStruct((count, width), BF16),
            jax.ShapeDtypeStruct((half, width), F32),
            jax.ShapeDtypeStruct((half, width), F32),
            jax.ShapeDtypeStruct((feat // n_z, count), F32),
        ),
        in_specs=[pl.BlockSpec(memory_space=VMEM)] * 6,
        out_specs=(pl.BlockSpec(memory_space=VMEM),) * 4,
        scratch_shapes=[
            VMEM((REACH, count, width), BF16),
            VMEM((REACH, count, width), BF16),
            VMEM((REACH, 1, count), jnp.int32),
            VMEM((count, width), F32),
            VMEM((REACH, count, width), F32),
            VMEM((ADJ_ROWS, count), BF16),
            VMEM((count, feat), BF16),
            VMEM((feat, count), F32),
            VMEM((feat, count), F32),
            VMEM((1, count), F32),
            VMEM((1, count), F32),
            VMEM((1, count), F32),
            VMEM((width, count), F32),
            VMEM((width, count), F32),
            VMEM((feat, width), F32),
            VMEM((feat, width), F32),
            VMEM((feat, count), F32),
            VMEM((feat, count), F32),
            VMEM((ADJ_ROWS, feat), BF16),
            VMEM((REACH, ADJ_ROWS, feat), BF16),
            VMEM((feat, count), BF16),
            VMEM((1, n_z, feat // n_z, count), BF16),
            VMEM((2, 2, half, width), BF16),
            VMEM((2, SIDE, half, width), BF16),
            VMEM((2, SIDE, half, width), BF16),
            VMEM((1, n_z, half, width), BF16),
            dma((REACH,)),
            dma((REACH,)),
            dma((2, 2)),
            dma((2, 2)),
            dma((2,)),
            dma((2,)),
            dma((2, n_z // 2, 2, 2)),
            dma((2, n_z // 2, 2, 2)),
            dma((2, 2)),
            dma((2, 2, n_z)),
            dma((REACH,)),
            dma((REACH,)),
            dma((1, n_z - 1)),
            dma((1, n_z)),
            dma((2, 1)),
            dma((2, 2)),
            dma((2, SIDE - 1)),
            dma((2, SIDE)),
            dma((2, SIDE - 1)),
            dma((2, SIDE)),
            dma((1, n_z - 1)),
            dma((1, n_z)),
        ],
        compiler_params=pltpu.CompilerParams(collective_id=0, has_side_effects=True),
        name="fused",
    )(queries, keys, values, codes, wq_t, wkey_t)


def solution(mesh):
    n_seq, n_z = mesh.shape["seq"], mesh.shape["tensor"]

    def shards(queries, keys, values, doc_ids, w_query, w_key):
        count, width = keys.shape
        student, gwq, gwk, kfg = fused(
            queries.reshape(count, width),
            keys,
            values,
            doc_ids.reshape(1, count),
            w_query[0].T,
            w_key.T,
            n_seq,
            n_z,
        )
        return student.reshape(queries.shape), gwq.T[None], gwk.T, kfg.T

    return jax.shard_map(
        shards,
        mesh=mesh,
        in_specs=(
            P("seq", "tensor", None),
            P("seq", None),
            P("seq", None),
            P("seq"),
            P("tensor", None, None),
            P(),
        ),
        out_specs=(P("seq", "tensor", None), P("tensor", None, None), P(), P("seq", "tensor")),
        check_vma=False,
    )
```

```python
import functools

import jax
import jax.numpy as jnp
from jax import lax
from jax.experimental import pallas as pl
from jax.experimental.pallas import tpu as pltpu
from jax.sharding import PartitionSpec as P

F32 = jnp.float32
BF16 = jnp.bfloat16
MESH = pl.DeviceIdType.MESH
VMEM = pltpu.VMEM

REACH = 4
SIDE = 4
NEGATIVE = -1e30
LOG2E = 1.4426950408889634
TILE = 256
ADJ_ROWS = 144


def dot(a, b, ca, cb):
    return lax.dot_general(a, b, (((ca,), (cb,)), ((), ())), preferred_element_type=F32)


def remote(src, dst, send_sem, recv_sem, **where):
    return pltpu.make_async_remote_copy(
        src_ref=src,
        dst_ref=dst,
        send_sem=send_sem,
        recv_sem=recv_sem,
        device_id=where,
        device_id_type=MESH,
    )


def signal(sem, **where):
    pl.semaphore_signal(sem, inc=1, device_id=where, device_id_type=MESH)


def features(rows, weights_t):
    logits = dot(weights_t, rows, 1, 1)
    up = jnp.exp(logits - jnp.max(logits, axis=0, keepdims=True))
    down = jnp.exp(jnp.min(logits, axis=0, keepdims=True) - logits)
    up = up / jnp.sum(up, axis=0, keepdims=True)
    down = down / jnp.sum(down, axis=0, keepdims=True)
    return jnp.concatenate([up, down], axis=0)


def features_back(feat, grad):
    half = feat.shape[0] // 2
    p, m, a, b = feat[:half], feat[half:], grad[:half], grad[half:]
    upper = p * (a - jnp.sum(a * p, axis=0, keepdims=True))
    lower = m * (b - jnp.sum(b * m, axis=0, keepdims=True))
    return upper - lower


def transposed(x):
    return x.astype(F32).T.astype(x.dtype)


def lane_copies(row, count):
    return jnp.broadcast_to(row, (count, row.shape[1])).T


def across(column, width):
    return jnp.concatenate([column] * (width // column.shape[1]), axis=1)


def fused_kernel(
    n_seq,
    n_z,
    q_hbm,
    k_hbm,
    v_hbm,
    c_hbm,
    wq_hbm,
    wkey_hbm,
    student_hbm,
    gwq_out,
    gwk_out,
    kfg_out,
    q_ref,
    k_ref,
    v_ref,
    c_ref,
    wq_ref,
    wkey_ref,
    student_ref,
    wk_ref,
    wv_ref,
    wc_ref,
    kcol_ref,
    fkf_ref,
    vt_ref,
    kfb_ref,
    kf_ref,
    qf_ref,
    top_ref,
    den_ref,
    acc_ref,
    num_ref,
    state_ref,
    ssum_ref,
    gqf_ref,
    gkf_ref,
    adj_ref,
    adj_in,
    spread_ref,
    gather_ref,
    core_ref,
    y_ref,
    x_ref,
    z_ref,
    load_sem,
    store_sem,
    code_send,
    code_recv,
    slice_send,
    slice_recv,
    pass_send,
    own_send,
    own_recv,
    ring_send,
    ring_recv,
    pair_send,
    pair_recv,
    adj_send,
    adj_recv,
    spread_send,
    spread_recv,
    core_send,
    core_recv,
    y_send,
    y_recv,
    x_send,
    x_recv,
    z_send,
    z_recv,
):
    count, width = k_ref.shape
    half = wkey_hbm.shape[0]
    total = float(count * n_seq)
    grad_scale = 2.0 / total
    factor = width**-0.5 * LOG2E
    s = lax.axis_index("seq")
    z = lax.axis_index("tensor")
    core = lax.rem(s, 2)
    partner = s + 1 - 2 * core
    y = lax.rem(s // 2, SIDE)
    x = s // (2 * SIDE)
    part = count // n_z
    share = 2 * half // n_z

    def later(d):
        return lax.rem(s + d, n_seq)

    def turn(d):
        return lax.rem(z + d + n_z, n_z)

    def along_y(i):
        return lax.rem(y + i, SIDE)

    def along_x(i):
        return lax.rem(x + i, SIDE)

    def seq_of(at_x, at_y):
        return (at_x * SIDE + at_y) * 2 + core

    def rows(p):
        return pl.ds(pl.multiple_of(p * part, part), part)

    loads = [
        pltpu.make_async_copy(far, near, load_sem.at[i])
        for i, (far, near) in enumerate(
            (
                (k_hbm, k_ref),
                (v_hbm, v_ref),
                (c_hbm, c_ref),
                (q_hbm, q_ref),
                (wq_hbm, wq_ref),
                (wkey_hbm, wkey_ref),
            )
        )
    ]
    for load in loads:
        load.start()

    barrier = pltpu.get_barrier_semaphore()
    for d in range(1, REACH + 1):
        signal(barrier, seq=later(n_seq - d))
        signal(barrier, seq=later(d))
    signal(barrier, seq=partner)
    for i in range(1, SIDE):
        signal(barrier, seq=seq_of(x, along_y(i)))
        signal(barrier, seq=seq_of(along_x(i), y))
    for i in range(1, n_z):
        signal(barrier, tensor=turn(i))
    for load in loads:
        load.wait()
    pl.semaphore_wait(barrier, 2 * REACH + 1 + 2 * (SIDE - 1) + n_z - 1)

    started = []

    def send(*args, **where):
        copy = remote(*args, **where)
        copy.start()
        started.append(copy)

    def arrive(here, send_sem, recv_sem):
        remote(here, here, send_sem, recv_sem, seq=partner).wait_recv()

    pairs = ((k_ref, wk_ref), (v_ref, wv_ref))
    slots = (3 - core, 2 - core)
    last = n_z // 2
    direct = (z, turn(last))

    def send_slice(j):
        for kv, (own, window) in enumerate(pairs):
            send(
                own.at[rows(direct[j])],
                window.at[2 - core, rows(direct[j])],
                slice_send.at[j, kv],
                slice_recv.at[j, core, kv],
                seq=later(3 - core),
            )

    def take_slice(j, i, kv):
        window = pairs[kv][1]
        here = window.at[slots[i], rows(direct[j])]
        arrive(here, slice_send.at[j, kv], slice_recv.at[j, i, kv])

        @pl.when(core == 1)
        def _():
            remote(
                here,
                window.at[3 - i, rows(direct[j])],
                pass_send.at[j, i, kv],
                slice_recv.at[j, i, kv],
                seq=later(1),
            ).start()

    send_slice(0)
    for d in range(1, REACH + 1):
        send(c_ref, wc_ref.at[d - 1], code_send.at[d - 1], code_recv.at[d - 1], seq=later(d))

    @pl.when(core == 0)
    def _():
        for kv, (own, window) in enumerate(pairs):
            remote(own, window.at[0], own_send.at[kv], own_recv.at[kv], seq=partner).start()

    def pass_to_partner(i, kv, piece, order):
        window = pairs[kv][1]

        def go(slot):
            remote(
                window.at[slots[i], rows(piece)],
                window.at[slot, rows(piece)],
                pair_send.at[i, kv],
                pair_recv.at[i, kv, order],
                seq=partner,
            ).start()

        if i == 1:
            go(3 - 3 * core)
        else:

            @pl.when(core == 1)
            def _():
                go(1)

    def from_partner(order, piece):
        for kv in range(2):
            here = pairs[kv][1].at[0, rows(piece)]
            arrive(here, pair_send.at[1, kv], pair_recv.at[1, kv, order])

            @pl.when(core == 0)
            def _():
                arrive(here, pair_send.at[0, kv], pair_recv.at[0, kv, order])

    def ring_copy(way, step, i, kv):
        here = pairs[kv][1].at[slots[i], rows(turn(1 - step) if way == 0 else turn(step - 1))]
        send(
            here,
            here,
            ring_send.at[way, step - 1, i, kv],
            ring_recv.at[way, step - 1, i, kv],
            tensor=turn(1 if way == 0 else -1),
        )

    def ring_step(step):
        for i in range(2):
            for kv in range(2):
                for way in range(2):
                    piece = turn(-step) if way == 0 else turn(step)
                    here = pairs[kv][1].at[slots[i], rows(piece)]
                    arrive(here, ring_send.at[way, step - 1, i, kv], ring_recv.at[way, step - 1, i, kv])
                    if step < last - 1:
                        ring_copy(way, step + 1, i, kv)
                    pass_to_partner(i, kv, piece, 2 * step - 1 + way)

    code = c_ref[...].astype(F32)
    leading = code[:, :1]
    lead = (code == leading).astype(F32)
    wkey_t = wkey_ref[...]
    kf = features(k_ref[...], wkey_t)
    kf_ref[...] = kf
    kft = kf.astype(BF16)
    kfb_ref[...] = kf.T.astype(BF16)
    qf = features(q_ref[...], wq_ref[...])
    qf_ref[...] = qf
    qft = qf.astype(BF16)
    vt_ref[:width] = transposed(v_ref[...])
    one = lax.broadcasted_iota(jnp.int32, (ADJ_ROWS - width, count), 0) == 0
    vt_ref[width:] = one.astype(F32).astype(BF16)
    kcol_ref[...] = lane_copies(code, width)

    def own_mask(start, limit):
        same = across(kcol_ref[:limit], TILE) == code[:, start:limit]
        key_at = lax.broadcasted_iota(jnp.int32, (limit, TILE), 0)
        query_at = lax.broadcasted_iota(jnp.int32, (limit, TILE), 1) + start
        return same & (key_at <= query_at)

    unit = (lax.broadcasted_iota(jnp.int32, (count, width), 1) == 0).astype(F32).astype(BF16)

    def own_tile(start):
        limit = start + TILE
        cols = slice(start, limit)
        same = across(kcol_ref[cols], limit) == code[:, :limit]
        key_at = lax.broadcasted_iota(jnp.int32, (TILE, limit), 1)
        query_at = lax.broadcasted_iota(jnp.int32, (TILE, limit), 0) + start
        scores = dot(q_ref[cols], k_ref[:limit], 1, 1)
        scores = jnp.where(same & (key_at <= query_at), scores * factor, NEGATIVE)
        top = jnp.broadcast_to(jnp.max(scores, axis=1, keepdims=True), (TILE, width))
        weights = jnp.exp2(scores - across(top, limit)).astype(BF16)
        top_ref[cols] = top
        acc_ref[cols] = dot(weights, jnp.concatenate([v_ref[:limit], unit[:limit]], axis=1), 1, 0)
        products = jnp.where(own_mask(start, limit), dot(kfb_ref[:limit], qft[:, cols], 1, 0), 0.0)
        den_ref[:, cols] = jnp.sum(products, axis=0, keepdims=True)
        num_ref[:, cols] = dot(vt_ref[:width, :limit], products.astype(BF16), 1, 0)

    def far_pieces(pieces):
        places = [(d, rows(p), p) for d in range(REACH) for p in pieces]
        keys = jnp.concatenate([wk_ref[d, r] for d, r, _ in places], axis=0)
        vals = jnp.concatenate([wv_ref[d, r] for d, r, _ in places], axis=0)
        codes = jnp.concatenate([wc_ref[d, :, r] for d, r, _ in places], axis=1).astype(F32)
        size = keys.shape[0]
        feat = features(keys, wkey_t)
        for n, (d, r, _) in enumerate(places):
            fkf_ref[d, :, r] = feat[:, n * part : (n + 1) * part]
        chosen = feat.astype(BF16).astype(F32) * (codes == leading).astype(F32)
        state_ref[...] += dot(chosen.astype(BF16), vals, 1, 0)
        ssum_ref[...] += jnp.broadcast_to(jnp.sum(chosen, axis=1, keepdims=True), ssum_ref.shape)
        wide = jnp.concatenate([vals, unit[:size]], axis=1)
        for start in range(0, count, TILE):
            cols = slice(start, start + TILE)
            scores = dot(q_ref[cols], keys, 1, 1)
            same = across(kcol_ref[cols], size) == codes
            scores = jnp.where(same, scores * factor, NEGATIVE)
            old = top_ref[cols]
            top = jnp.maximum(old, jnp.max(scores, axis=1, keepdims=True))
            weights = jnp.exp2(scores - across(top, size)).astype(BF16)
            shrink = jnp.exp2(old - top)
            top_ref[cols] = top
            acc_ref[cols] = acc_ref[cols] * across(shrink, 2 * width) + dot(weights, wide, 1, 0)

    for start in range(0, count // 2, TILE):
        own_tile(start)
    state_ref[...] = jnp.zeros_like(state_ref)
    ssum_ref[...] = jnp.zeros_like(ssum_ref)
    for i in range(2):
        for kv in range(2):
            take_slice(0, i, kv)
            for way in range(2):
                ring_copy(way, 1, i, kv)
            pass_to_partner(i, kv, z, 0)
    send_slice(1)
    for start in range(count // 2, count, TILE):
        own_tile(start)
    for d in range(REACH):
        arrive(wc_ref.at[d], code_send.at[d], code_recv.at[d])

    @pl.when(core == 1)
    def _():
        for kv in range(2):
            arrive(pairs[kv][1].at[0], own_send.at[kv], own_recv.at[kv])

    def both_from_partner(step):
        from_partner(2 * step - 1, turn(-step))
        from_partner(2 * step, turn(step))

    ring_step(1)
    from_partner(0, z)
    far_pieces((z,))
    for i in range(2):
        for kv in range(2):
            take_slice(1, i, kv)
            pass_to_partner(i, kv, turn(last), n_z - 1)
    ring_step(2)
    both_from_partner(1)
    far_pieces((turn(-1), turn(1)))
    from_partner(n_z - 1, turn(last))
    far_pieces((turn(last),))
    ring_step(3)
    both_from_partner(2)
    far_pieces((turn(-2), turn(2)))
    both_from_partner(3)
    far_pieces((turn(-3), turn(3)))

    state = state_ref[...]
    state_sum = ssum_ref[:, :1]
    acc = acc_ref[...]
    teacher = (acc[:, :width] / acc[:, width : width + 1]).T
    numerator = num_ref[...] + lead * dot(state.T.astype(BF16), qft, 1, 0)
    denominator = den_ref[...] + lead * jnp.sum(
        qft.astype(F32) * state_sum, axis=0, keepdims=True
    )
    estimate = numerator / denominator
    grad_out = grad_scale * (estimate - teacher)
    grad_num = grad_out / denominator
    grad_den = -jnp.sum(grad_out * estimate, axis=0, keepdims=True) / denominator
    gnt = grad_num.astype(BF16)

    row = lax.broadcasted_iota(jnp.int32, (ADJ_ROWS - width, count), 0)
    tail = jnp.where(row == 0, grad_den * lead, 0.0)
    masked = jnp.concatenate([grad_num * lead, tail], axis=0).astype(BF16)
    adjoint = dot(masked, qft, 1, 1)
    mark = lax.broadcasted_iota(jnp.int32, adjoint.shape, 0)
    adj_ref[...] = jnp.where(mark == width + 1, leading, adjoint).astype(BF16)
    for d in range(1, REACH + 1):
        send(
            adj_ref,
            adj_in.at[d - 1],
            adj_send.at[d - 1],
            adj_recv.at[d - 1],
            seq=later(n_seq - d),
        )

    gqf_ref[...] = lead * (dot(state.astype(BF16), gnt, 1, 0) + state_sum * grad_den)
    for start in range(0, count, TILE):
        limit = start + TILE
        cols = slice(start, limit)
        grad_prod = dot(v_ref[:limit], gnt[:, cols], 1, 0) + grad_den[:, cols]
        grad_prod = jnp.where(own_mask(start, limit), grad_prod, 0.0).astype(BF16)
        gqf_ref[:, cols] += dot(kft[:, :limit], grad_prod, 1, 0)
        piece = dot(qft[:, cols], grad_prod, 1, 1)
        if start:
            gkf_ref[:, :start] += piece[:, :start]
        gkf_ref[:, cols] = piece[:, start:]

    def wait(ref, which, at, send_sems, recv_sems):
        here = ref.at[which, at]
        arrive(here, send_sems.at[which, 0], recv_sems.at[which, at])

    def summed(ref, which):
        result = ref[which, 0].astype(F32)
        for i in range(1, ref.shape[1]):
            result = result + ref[which, i].astype(F32)
        return result

    def over_core(which, value):
        core_ref[which, core] = value.astype(BF16)
        here = core_ref.at[which, core]
        send(here, here, core_send.at[which, 0], core_recv.at[which, core], seq=partner)

    def over_y(which):
        wait(core_ref, which, 1 - core, core_send, core_recv)
        y_ref[which, y] = summed(core_ref, which).astype(BF16)
        here = y_ref.at[which, y]
        for i in range(1, SIDE):
            to = seq_of(x, along_y(i))
            send(here, here, y_send.at[which, i - 1], y_recv.at[which, y], seq=to)

    def over_x(which):
        for i in range(1, SIDE):
            wait(y_ref, which, along_y(i), y_send, y_recv)
        x_ref[which, x] = summed(y_ref, which).astype(BF16)
        here = x_ref.at[which, x]
        for i in range(1, SIDE):
            to = seq_of(along_x(i), y)
            send(here, here, x_send.at[which, i - 1], x_recv.at[which, x], seq=to)

    def over_seq(which):
        for i in range(1, SIDE):
            wait(x_ref, which, along_x(i), x_send, x_recv)
        return summed(x_ref, which)

    grad_aq = features_back(qf_ref[...], gqf_ref[...]).astype(BF16)
    over_core(0, dot(grad_aq, q_ref[...], 1, 0))
    student_ref[...] = estimate.T.astype(BF16)
    store = pltpu.make_async_copy(student_ref, student_hbm, store_sem.at[0])
    store.start()

    grad_ak = features_back(kf_ref[...], gkf_ref[...]).astype(BF16)
    grad_wk = dot(grad_ak, k_ref[...], 1, 0)
    adjoint_t = adjoint.T
    adjoint_b = adjoint_t[:, :width].astype(BF16)
    adjoint_sum = adjoint_t[:, width : width + 1]
    for d in range(REACH):
        met = (wc_ref[d].astype(F32) == leading).astype(F32)
        caused = (dot(adjoint_b, wv_ref[d], 1, 1) + adjoint_sum) * met
        grad_ak = features_back(fkf_ref[d], caused).astype(BF16)
        grad_wk = grad_wk + dot(grad_ak, wk_ref[d], 1, 0)
    over_core(1, grad_wk)
    over_y(0)

    final = code[:, count - 1 :]
    back = (code == final).astype(F32)
    entering = jnp.zeros(adj_ref.shape, F32)
    for d in range(REACH):
        arrive(adj_in.at[d], adj_send.at[d], adj_recv.at[d])
        arrived = adj_in[d].astype(F32)
        entering = entering + jnp.where(arrived[width + 1 : width + 2] == final, arrived, 0.0)
    over_y(1)
    added = dot(entering.T.astype(BF16), vt_ref[...], 1, 0)
    grad_kf = gkf_ref[...] + back * added
    spread_ref[...] = (grad_kf * total).astype(BF16)
    for i in range(1, n_z):
        to = turn(i)
        send(
            spread_ref.at[pl.ds(pl.multiple_of(to * share, share), share)],
            gather_ref.at[0, z],
            spread_send.at[0, i - 1],
            spread_recv.at[0, z],
            tensor=to,
        )
    gather_ref[0, z] = spread_ref[pl.ds(pl.multiple_of(z * share, share), share)]

    over_x(0)
    over_x(1)
    z_ref[0, z] = over_seq(1).astype(BF16)
    here = z_ref.at[0, z]
    for i in range(1, n_z):
        send(here, here, z_send.at[0, i - 1], z_recv.at[0, z], tensor=turn(i))
    gwq_out[...] = over_seq(0)
    for i in range(1, n_z):
        wait(gather_ref, 0, turn(i), spread_send, spread_recv)
    kfg_out[...] = summed(gather_ref, 0)
    for i in range(1, n_z):
        wait(z_ref, 0, turn(i), z_send, z_recv)
    gwk_out[...] = summed(z_ref, 0)

    store.wait()
    for copy in started:
        copy.wait_send()
    for kv, (own, window) in enumerate(pairs):
        block = window.at[0]
        remote(block, block, pair_send.at[1, kv], own_recv.at[kv], seq=partner).wait_send()

        @pl.when(core == 1)
        def _():
            remote(block, block, pair_send.at[0, kv], own_recv.at[kv], seq=partner).wait_send()
            for j in range(2):
                for i in range(2):
                    here = window.at[0, rows(z)]
                    remote(here, here, pass_send.at[j, i, kv], own_recv.at[kv], seq=partner).wait_send()

        @pl.when(core == 0)
        def _():
            remote(own, block, own_send.at[kv], own_recv.at[kv], seq=partner).wait_send()


def fused(queries, keys, values, codes, wq_t, wkey_t, n_seq, n_z):
    count, width = keys.shape
    half = wkey_t.shape[0]
    feat = 2 * half
    dma = pltpu.SemaphoreType.DMA
    return pl.pallas_call(
        functools.partial(fused_kernel, n_seq, n_z),
        out_shape=(
            jax.ShapeDtypeStruct((count, width), BF16),
            jax.ShapeDtypeStruct((half, width), F32),
            jax.ShapeDtypeStruct((half, width), F32),
            jax.ShapeDtypeStruct((feat // n_z, count), F32),
        ),
        in_specs=[pl.BlockSpec(memory_space=pl.ANY)] * 6,
        out_specs=(
            pl.BlockSpec(memory_space=pl.ANY),
            *[pl.BlockSpec(memory_space=VMEM)] * 3,
        ),
        scratch_shapes=[
            VMEM((count, width), BF16),
            VMEM((count, width), BF16),
            VMEM((count, width), BF16),
            VMEM((1, count), jnp.int32),
            VMEM((half, width), BF16),
            VMEM((half, width), BF16),
            VMEM((count, width), BF16),
            VMEM((REACH, count, width), BF16),
            VMEM((REACH, count, width), BF16),
            VMEM((REACH, 1, count), jnp.int32),
            VMEM((count, width), F32),
            VMEM((REACH, feat, count), F32),
            VMEM((ADJ_ROWS, count), BF16),
            VMEM((count, feat), BF16),
            VMEM((feat, count), F32),
            VMEM((feat, count), F32),
            VMEM((count, width), F32),
            VMEM((1, count), F32),
            VMEM((count, 2 * width), F32),
            VMEM((width, count), F32),
            VMEM((feat, width), F32),
            VMEM((feat, width), F32),
            VMEM((feat, count), F32),
            VMEM((feat, count), F32),
            VMEM((ADJ_ROWS, feat), BF16),
            VMEM((REACH, ADJ_ROWS, feat), BF16),
            VMEM((feat, count), BF16),
            VMEM((1, n_z, feat // n_z, count), BF16),
            VMEM((2, 2, half, width), BF16),
            VMEM((2, SIDE, half, width), BF16),
            VMEM((2, SIDE, half, width), BF16),
            VMEM((1, n_z, half, width), BF16),
            dma((6,)),
            dma((1,)),
            dma((REACH,)),
            dma((REACH,)),
            dma((2, 2)),
            dma((2, 2, 2)),
            dma((2, 2, 2)),
            dma((2,)),
            dma((2,)),
            dma((2, n_z // 2 - 1, 2, 2)),
            dma((2, n_z // 2 - 1, 2, 2)),
            dma((2, 2)),
            dma((2, 2, n_z)),
            dma((REACH,)),
            dma((REACH,)),
            dma((1, n_z - 1)),
            dma((1, n_z)),
            dma((2, 1)),
            dma((2, 2)),
            dma((2, SIDE - 1)),
            dma((2, SIDE)),
            dma((2, SIDE - 1)),
            dma((2, SIDE)),
            dma((1, n_z - 1)),
            dma((1, n_z)),
        ],
        compiler_params=pltpu.CompilerParams(collective_id=0, has_side_effects=True),
        name="fused",
    )(queries, keys, values, codes, wq_t, wkey_t)


def solution(mesh):
    n_seq, n_z = mesh.shape["seq"], mesh.shape["tensor"]

    def shards(queries, keys, values, doc_ids, w_query, w_key):
        count, width = keys.shape
        student, gwq, gwk, kfg = fused(
            queries.reshape(count, width),
            keys,
            values,
            doc_ids.reshape(1, count),
            w_query[0].T,
            w_key.T,
            n_seq,
            n_z,
        )
        return student.reshape(queries.shape), gwq.T[None], gwk.T, kfg.T

    return jax.shard_map(
        shards,
        mesh=mesh,
        in_specs=(
            P("seq", "tensor", None),
            P("seq", None),
            P("seq", None),
            P("seq"),
            P("tensor", None, None),
            P(),
        ),
        out_specs=(P("seq", "tensor", None), P("tensor", None, None), P(), P("seq", "tensor")),
        check_vma=False,
    )
```

```python
import functools

import jax
import jax.numpy as jnp
from jax import lax
from jax.experimental import pallas as pl
from jax.experimental.pallas import tpu as pltpu
from jax.sharding import PartitionSpec as P

F32 = jnp.float32
BF16 = jnp.bfloat16
MESH = pl.DeviceIdType.MESH
VMEM = pltpu.VMEM

REACH = 4
SIDE = 4
NEGATIVE = -1e30
LOG2E = 1.4426950408889634
TILE = 256
ADJ_ROWS = 144


def dot(a, b, ca, cb):
    return lax.dot_general(a, b, (((ca,), (cb,)), ((), ())), preferred_element_type=F32)


def remote(src, dst, send_sem, recv_sem, **where):
    return pltpu.make_async_remote_copy(
        src_ref=src,
        dst_ref=dst,
        send_sem=send_sem,
        recv_sem=recv_sem,
        device_id=where,
        device_id_type=MESH,
    )


def signal(sem, **where):
    pl.semaphore_signal(sem, inc=1, device_id=where, device_id_type=MESH)


def features(rows, weights_t):
    logits = dot(weights_t, rows, 1, 1)
    up = jnp.exp(logits - jnp.max(logits, axis=0, keepdims=True))
    down = jnp.exp(jnp.min(logits, axis=0, keepdims=True) - logits)
    up = up / jnp.sum(up, axis=0, keepdims=True)
    down = down / jnp.sum(down, axis=0, keepdims=True)
    return jnp.concatenate([up, down], axis=0)


def features_back(feat, grad):
    half = feat.shape[0] // 2
    p, m, a, b = feat[:half], feat[half:], grad[:half], grad[half:]
    upper = p * (a - jnp.sum(a * p, axis=0, keepdims=True))
    lower = m * (b - jnp.sum(b * m, axis=0, keepdims=True))
    return upper - lower


def transposed(x):
    return x.astype(F32).T.astype(x.dtype)


def lane_copies(row, count):
    return jnp.broadcast_to(row, (count, row.shape[1])).T


def across(column, width):
    return jnp.concatenate([column] * (width // column.shape[1]), axis=1)


def fused_kernel(
    n_seq,
    n_z,
    q_hbm,
    k_hbm,
    v_hbm,
    c_hbm,
    wq_hbm,
    wkey_hbm,
    student_hbm,
    gwq_out,
    gwk_out,
    kfg_out,
    q_ref,
    k_ref,
    v_ref,
    c_ref,
    wq_ref,
    wkey_ref,
    student_ref,
    wk_ref,
    wv_ref,
    wc_ref,
    kcol_ref,
    fkf_ref,
    vt_ref,
    kfb_ref,
    kf_ref,
    qf_ref,
    top_ref,
    den_ref,
    acc_ref,
    num_ref,
    state_ref,
    ssum_ref,
    gqf_ref,
    gkf_ref,
    adj_ref,
    adj_in,
    spread_ref,
    gather_ref,
    core_ref,
    y_ref,
    x_ref,
    z_ref,
    load_sem,
    store_sem,
    code_send,
    code_recv,
    slice_send,
    slice_recv,
    pass_send,
    own_send,
    own_recv,
    ring_send,
    ring_recv,
    pair_send,
    pair_recv,
    adj_send,
    adj_recv,
    spread_send,
    spread_recv,
    core_send,
    core_recv,
    y_send,
    y_recv,
    x_send,
    x_recv,
    z_send,
    z_recv,
):
    count, width = k_ref.shape
    half = wkey_hbm.shape[0]
    total = float(count * n_seq)
    grad_scale = 2.0 / total
    factor = width**-0.5 * LOG2E
    s = lax.axis_index("seq")
    z = lax.axis_index("tensor")
    core = lax.rem(s, 2)
    partner = s + 1 - 2 * core
    y = lax.rem(s // 2, SIDE)
    x = s // (2 * SIDE)
    part = count // n_z
    share = 2 * half // n_z

    def later(d):
        return lax.rem(s + d, n_seq)

    def turn(d):
        return lax.rem(z + d + n_z, n_z)

    def along_y(i):
        return lax.rem(y + i, SIDE)

    def along_x(i):
        return lax.rem(x + i, SIDE)

    def seq_of(at_x, at_y):
        return (at_x * SIDE + at_y) * 2 + core

    def rows(p):
        return pl.ds(pl.multiple_of(p * part, part), part)

    loads = [
        pltpu.make_async_copy(far, near, load_sem.at[i])
        for i, (far, near) in enumerate(
            (
                (k_hbm, k_ref),
                (v_hbm, v_ref),
                (c_hbm, c_ref),
                (q_hbm, q_ref),
                (wq_hbm, wq_ref),
                (wkey_hbm, wkey_ref),
            )
        )
    ]
    for load in loads:
        load.start()

    barrier = pltpu.get_barrier_semaphore()
    for d in range(1, REACH + 1):
        signal(barrier, seq=later(n_seq - d))
        signal(barrier, seq=later(d))
    signal(barrier, seq=partner)
    for i in range(1, SIDE):
        signal(barrier, seq=seq_of(x, along_y(i)))
        signal(barrier, seq=seq_of(along_x(i), y))
    for i in range(1, n_z):
        signal(barrier, tensor=turn(i))
    for load in loads[:3]:
        load.wait()
    pl.semaphore_wait(barrier, 2 * REACH + 1 + 2 * (SIDE - 1) + n_z - 1)

    started = []

    def send(*args, **where):
        copy = remote(*args, **where)
        copy.start()
        started.append(copy)

    def arrive(here, send_sem, recv_sem):
        remote(here, here, send_sem, recv_sem, seq=partner).wait_recv()

    pairs = ((k_ref, wk_ref), (v_ref, wv_ref))
    slots = (3 - core, 2 - core)
    last = n_z // 2
    direct = (z, turn(last), turn(last - 1), turn(1 - last))

    def send_slice(j):
        for kv, (own, window) in enumerate(pairs):
            send(
                own.at[rows(direct[j])],
                window.at[2 - core, rows(direct[j])],
                slice_send.at[j, kv],
                slice_recv.at[j, core, kv],
                seq=later(3 - core),
            )

    def take_slice(j, i, kv):
        window = pairs[kv][1]
        here = window.at[slots[i], rows(direct[j])]
        arrive(here, slice_send.at[j, kv], slice_recv.at[j, i, kv])

        @pl.when(core == 1)
        def _():
            remote(
                here,
                window.at[3 - i, rows(direct[j])],
                pass_send.at[j, i, kv],
                slice_recv.at[j, i, kv],
                seq=later(1),
            ).start()

    send_slice(0)
    send_slice(1)
    for d in range(1, REACH + 1):
        send(c_ref, wc_ref.at[d - 1], code_send.at[d - 1], code_recv.at[d - 1], seq=later(d))

    @pl.when(core == 0)
    def _():
        for kv, (own, window) in enumerate(pairs):
            remote(own, window.at[0], own_send.at[kv], own_recv.at[kv], seq=partner).start()

    def pass_to_partner(i, kv, piece, order):
        window = pairs[kv][1]

        def go(slot):
            remote(
                window.at[slots[i], rows(piece)],
                window.at[slot, rows(piece)],
                pair_send.at[i, kv],
                pair_recv.at[i, kv, order],
                seq=partner,
            ).start()

        if i == 1:
            go(3 - 3 * core)
        else:

            @pl.when(core == 1)
            def _():
                go(1)

    def from_partner(order, piece):
        for kv in range(2):
            here = pairs[kv][1].at[0, rows(piece)]
            arrive(here, pair_send.at[1, kv], pair_recv.at[1, kv, order])

            @pl.when(core == 0)
            def _():
                arrive(here, pair_send.at[0, kv], pair_recv.at[0, kv, order])

    def ring_copy(way, step, i, kv):
        here = pairs[kv][1].at[slots[i], rows(turn(1 - step) if way == 0 else turn(step - 1))]
        send(
            here,
            here,
            ring_send.at[way, step - 1, i, kv],
            ring_recv.at[way, step - 1, i, kv],
            tensor=turn(1 if way == 0 else -1),
        )

    def ring_step(step):
        for i in range(2):
            for kv in range(2):
                for way in range(2):
                    piece = turn(-step) if way == 0 else turn(step)
                    here = pairs[kv][1].at[slots[i], rows(piece)]
                    arrive(here, ring_send.at[way, step - 1, i, kv], ring_recv.at[way, step - 1, i, kv])
                    if step < last - 2:
                        ring_copy(way, step + 1, i, kv)
                    pass_to_partner(i, kv, piece, 2 * step - 1 + way)

    for load in loads[3:]:
        load.wait()
    code = c_ref[...].astype(F32)
    leading = code[:, :1]
    lead = (code == leading).astype(F32)
    wkey_t = wkey_ref[...]
    kf = features(k_ref[...], wkey_t)
    kf_ref[...] = kf
    kft = kf.astype(BF16)
    kfb_ref[...] = kf.T.astype(BF16)
    qf = features(q_ref[...], wq_ref[...])
    qf_ref[...] = qf
    qft = qf.astype(BF16)
    vt_ref[:width] = transposed(v_ref[...])
    one = lax.broadcasted_iota(jnp.int32, (ADJ_ROWS - width, count), 0) == 0
    vt_ref[width:] = one.astype(F32).astype(BF16)
    kcol_ref[...] = lane_copies(code, width)

    def own_mask(start, limit):
        same = across(kcol_ref[:limit], TILE) == code[:, start:limit]
        key_at = lax.broadcasted_iota(jnp.int32, (limit, TILE), 0)
        query_at = lax.broadcasted_iota(jnp.int32, (limit, TILE), 1) + start
        return same & (key_at <= query_at)

    unit = (lax.broadcasted_iota(jnp.int32, (count, width), 1) == 0).astype(F32).astype(BF16)

    def own_tile(start):
        limit = start + TILE
        cols = slice(start, limit)
        same = across(kcol_ref[cols], limit) == code[:, :limit]
        key_at = lax.broadcasted_iota(jnp.int32, (TILE, limit), 1)
        query_at = lax.broadcasted_iota(jnp.int32, (TILE, limit), 0) + start
        scores = dot(q_ref[cols], k_ref[:limit], 1, 1)
        scores = jnp.where(same & (key_at <= query_at), scores * factor, NEGATIVE)
        top = jnp.broadcast_to(jnp.max(scores, axis=1, keepdims=True), (TILE, width))
        weights = jnp.exp2(scores - across(top, limit)).astype(BF16)
        top_ref[cols] = top
        acc_ref[cols] = dot(weights, jnp.concatenate([v_ref[:limit], unit[:limit]], axis=1), 1, 0)
        products = jnp.where(own_mask(start, limit), dot(kfb_ref[:limit], qft[:, cols], 1, 0), 0.0)
        den_ref[:, cols] = jnp.sum(products, axis=0, keepdims=True)
        num_ref[:, cols] = dot(vt_ref[:width, :limit], products.astype(BF16), 1, 0)

    def far_pieces(pieces):
        places = [(d, rows(p), p) for d in range(REACH) for p in pieces]
        keys = jnp.concatenate([wk_ref[d, r] for d, r, _ in places], axis=0)
        vals = jnp.concatenate([wv_ref[d, r] for d, r, _ in places], axis=0)
        codes = jnp.concatenate([wc_ref[d, :, r] for d, r, _ in places], axis=1).astype(F32)
        size = keys.shape[0]
        feat = features(keys, wkey_t)
        for n, (d, r, _) in enumerate(places):
            fkf_ref[d, :, r] = feat[:, n * part : (n + 1) * part]
        chosen = feat.astype(BF16).astype(F32) * (codes == leading).astype(F32)
        state_ref[...] += dot(chosen.astype(BF16), vals, 1, 0)
        ssum_ref[...] += jnp.broadcast_to(jnp.sum(chosen, axis=1, keepdims=True), ssum_ref.shape)
        wide = jnp.concatenate([vals, unit[:size]], axis=1)
        for start in range(0, count, TILE):
            cols = slice(start, start + TILE)
            scores = dot(q_ref[cols], keys, 1, 1)
            same = across(kcol_ref[cols], size) == codes
            scores = jnp.where(same, scores * factor, NEGATIVE)
            old = top_ref[cols]
            top = jnp.maximum(old, jnp.max(scores, axis=1, keepdims=True))
            weights = jnp.exp2(scores - across(top, size)).astype(BF16)
            shrink = jnp.exp2(old - top)
            top_ref[cols] = top
            acc_ref[cols] = acc_ref[cols] * across(shrink, 2 * width) + dot(weights, wide, 1, 0)

    for start in range(0, count // 2, TILE):
        own_tile(start)
    state_ref[...] = jnp.zeros_like(state_ref)
    ssum_ref[...] = jnp.zeros_like(ssum_ref)
    for i in range(2):
        for kv in range(2):
            take_slice(0, i, kv)
            for way in range(2):
                ring_copy(way, 1, i, kv)
            pass_to_partner(i, kv, z, 0)
    send_slice(2)
    for start in range(count // 2, count, TILE):
        own_tile(start)
    for d in range(REACH):
        arrive(wc_ref.at[d], code_send.at[d], code_recv.at[d])

    @pl.when(core == 1)
    def _():
        for kv in range(2):
            arrive(pairs[kv][1].at[0], own_send.at[kv], own_recv.at[kv])

    def both_from_partner(step):
        from_partner(2 * step - 1, turn(-step))
        from_partner(2 * step, turn(step))

    def take_direct(j, order):
        for i in range(2):
            for kv in range(2):
                take_slice(j, i, kv)
                pass_to_partner(i, kv, direct[j], order)

    take_direct(1, n_z - 1)
    send_slice(3)
    ring_step(1)
    from_partner(0, z)
    far_pieces((z,))
    take_direct(2, n_z - 2)
    from_partner(n_z - 1, turn(last))
    far_pieces((turn(last),))
    ring_step(2)
    both_from_partner(1)
    far_pieces((turn(-1), turn(1)))
    take_direct(3, n_z - 3)
    both_from_partner(2)
    far_pieces((turn(-2), turn(2)))
    both_from_partner(3)
    far_pieces((turn(-3), turn(3)))

    state = state_ref[...]
    state_sum = ssum_ref[:, :1]
    acc = acc_ref[...]
    teacher = (acc[:, :width] / acc[:, width : width + 1]).T
    numerator = num_ref[...] + lead * dot(state.T.astype(BF16), qft, 1, 0)
    denominator = den_ref[...] + lead * jnp.sum(
        qft.astype(F32) * state_sum, axis=0, keepdims=True
    )
    estimate = numerator / denominator
    grad_out = grad_scale * (estimate - teacher)
    grad_num = grad_out / denominator
    grad_den = -jnp.sum(grad_out * estimate, axis=0, keepdims=True) / denominator
    gnt = grad_num.astype(BF16)

    row = lax.broadcasted_iota(jnp.int32, (ADJ_ROWS - width, count), 0)
    tail = jnp.where(row == 0, grad_den * lead, 0.0)
    masked = jnp.concatenate([grad_num * lead, tail], axis=0).astype(BF16)
    adjoint = dot(masked, qft, 1, 1)
    mark = lax.broadcasted_iota(jnp.int32, adjoint.shape, 0)
    adj_ref[...] = jnp.where(mark == width + 1, leading, adjoint).astype(BF16)
    for d in range(1, REACH + 1):
        send(
            adj_ref,
            adj_in.at[d - 1],
            adj_send.at[d - 1],
            adj_recv.at[d - 1],
            seq=later(n_seq - d),
        )

    gqf_ref[...] = lead * (dot(state.astype(BF16), gnt, 1, 0) + state_sum * grad_den)
    for start in range(0, count, TILE):
        limit = start + TILE
        cols = slice(start, limit)
        grad_prod = dot(v_ref[:limit], gnt[:, cols], 1, 0) + grad_den[:, cols]
        grad_prod = jnp.where(own_mask(start, limit), grad_prod, 0.0).astype(BF16)
        gqf_ref[:, cols] += dot(kft[:, :limit], grad_prod, 1, 0)
        piece = dot(qft[:, cols], grad_prod, 1, 1)
        if start:
            gkf_ref[:, :start] += piece[:, :start]
        gkf_ref[:, cols] = piece[:, start:]

    def wait(ref, which, at, send_sems, recv_sems):
        here = ref.at[which, at]
        arrive(here, send_sems.at[which, 0], recv_sems.at[which, at])

    def summed(ref, which):
        result = ref[which, 0].astype(F32)
        for i in range(1, ref.shape[1]):
            result = result + ref[which, i].astype(F32)
        return result

    def over_core(which, value):
        core_ref[which, core] = value.astype(BF16)
        here = core_ref.at[which, core]
        send(here, here, core_send.at[which, 0], core_recv.at[which, core], seq=partner)

    def over_y(which):
        wait(core_ref, which, 1 - core, core_send, core_recv)
        y_ref[which, y] = summed(core_ref, which).astype(BF16)
        here = y_ref.at[which, y]
        for i in range(1, SIDE):
            to = seq_of(x, along_y(i))
            send(here, here, y_send.at[which, i - 1], y_recv.at[which, y], seq=to)

    def over_x(which):
        for i in range(1, SIDE):
            wait(y_ref, which, along_y(i), y_send, y_recv)
        x_ref[which, x] = summed(y_ref, which).astype(BF16)
        here = x_ref.at[which, x]
        for i in range(1, SIDE):
            to = seq_of(along_x(i), y)
            send(here, here, x_send.at[which, i - 1], x_recv.at[which, x], seq=to)

    def over_seq(which):
        for i in range(1, SIDE):
            wait(x_ref, which, along_x(i), x_send, x_recv)
        return summed(x_ref, which)

    grad_ak = features_back(kf_ref[...], gkf_ref[...]).astype(BF16)
    grad_wk = dot(grad_ak, k_ref[...], 1, 0)
    adjoint_t = adjoint.T
    adjoint_b = adjoint_t[:, :width].astype(BF16)
    adjoint_sum = adjoint_t[:, width : width + 1]
    for d in range(REACH):
        met = (wc_ref[d].astype(F32) == leading).astype(F32)
        caused = (dot(adjoint_b, wv_ref[d], 1, 1) + adjoint_sum) * met
        grad_ak = features_back(fkf_ref[d], caused).astype(BF16)
        grad_wk = grad_wk + dot(grad_ak, wk_ref[d], 1, 0)
    over_core(1, grad_wk)

    grad_aq = features_back(qf_ref[...], gqf_ref[...]).astype(BF16)
    over_core(0, dot(grad_aq, q_ref[...], 1, 0))
    student_ref[...] = estimate.T.astype(BF16)
    store = pltpu.make_async_copy(student_ref, student_hbm, store_sem.at[0])
    store.start()
    over_y(1)

    final = code[:, count - 1 :]
    back = (code == final).astype(F32)
    entering = jnp.zeros(adj_ref.shape, F32)
    for d in range(REACH):
        arrive(adj_in.at[d], adj_send.at[d], adj_recv.at[d])
        arrived = adj_in[d].astype(F32)
        entering = entering + jnp.where(arrived[width + 1 : width + 2] == final, arrived, 0.0)
    added = dot(entering.T.astype(BF16), vt_ref[...], 1, 0)
    grad_kf = gkf_ref[...] + back * added
    spread_ref[...] = (grad_kf * total).astype(BF16)
    for i in range(1, n_z):
        to = turn(i)
        send(
            spread_ref.at[pl.ds(pl.multiple_of(to * share, share), share)],
            gather_ref.at[0, z],
            spread_send.at[0, i - 1],
            spread_recv.at[0, z],
            tensor=to,
        )
    gather_ref[0, z] = spread_ref[pl.ds(pl.multiple_of(z * share, share), share)]

    over_x(1)
    over_y(0)
    z_ref[0, z] = over_seq(1).astype(BF16)
    here = z_ref.at[0, z]
    for i in range(1, n_z):
        send(here, here, z_send.at[0, i - 1], z_recv.at[0, z], tensor=turn(i))
    over_x(0)
    gwq_out[...] = over_seq(0)
    for i in range(1, n_z):
        wait(gather_ref, 0, turn(i), spread_send, spread_recv)
    kfg_out[...] = summed(gather_ref, 0)
    for i in range(1, n_z):
        wait(z_ref, 0, turn(i), z_send, z_recv)
    gwk_out[...] = summed(z_ref, 0)

    store.wait()
    for copy in started:
        copy.wait_send()
    for kv, (own, window) in enumerate(pairs):
        block = window.at[0]
        remote(block, block, pair_send.at[1, kv], own_recv.at[kv], seq=partner).wait_send()

        @pl.when(core == 1)
        def _():
            remote(block, block, pair_send.at[0, kv], own_recv.at[kv], seq=partner).wait_send()
            for j in range(len(direct)):
                for i in range(2):
                    here = window.at[0, rows(z)]
                    remote(here, here, pass_send.at[j, i, kv], own_recv.at[kv], seq=partner).wait_send()

        @pl.when(core == 0)
        def _():
            remote(own, block, own_send.at[kv], own_recv.at[kv], seq=partner).wait_send()


def fused(queries, keys, values, codes, wq_t, wkey_t, n_seq, n_z):
    count, width = keys.shape
    half = wkey_t.shape[0]
    feat = 2 * half
    dma = pltpu.SemaphoreType.DMA
    return pl.pallas_call(
        functools.partial(fused_kernel, n_seq, n_z),
        out_shape=(
            jax.ShapeDtypeStruct((count, width), BF16),
            jax.ShapeDtypeStruct((half, width), F32),
            jax.ShapeDtypeStruct((half, width), F32),
            jax.ShapeDtypeStruct((feat // n_z, count), F32),
        ),
        in_specs=[pl.BlockSpec(memory_space=pl.ANY)] * 6,
        out_specs=(
            pl.BlockSpec(memory_space=pl.ANY),
            *[pl.BlockSpec(memory_space=VMEM)] * 3,
        ),
        scratch_shapes=[
            VMEM((count, width), BF16),
            VMEM((count, width), BF16),
            VMEM((count, width), BF16),
            VMEM((1, count), jnp.int32),
            VMEM((half, width), BF16),
            VMEM((half, width), BF16),
            VMEM((count, width), BF16),
            VMEM((REACH, count, width), BF16),
            VMEM((REACH, count, width), BF16),
            VMEM((REACH, 1, count), jnp.int32),
            VMEM((count, width), F32),
            VMEM((REACH, feat, count), F32),
            VMEM((ADJ_ROWS, count), BF16),
            VMEM((count, feat), BF16),
            VMEM((feat, count), F32),
            VMEM((feat, count), F32),
            VMEM((count, width), F32),
            VMEM((1, count), F32),
            VMEM((count, 2 * width), F32),
            VMEM((width, count), F32),
            VMEM((feat, width), F32),
            VMEM((feat, width), F32),
            VMEM((feat, count), F32),
            VMEM((feat, count), F32),
            VMEM((ADJ_ROWS, feat), BF16),
            VMEM((REACH, ADJ_ROWS, feat), BF16),
            VMEM((feat, count), BF16),
            VMEM((1, n_z, feat // n_z, count), BF16),
            VMEM((2, 2, half, width), BF16),
            VMEM((2, SIDE, half, width), BF16),
            VMEM((2, SIDE, half, width), BF16),
            VMEM((1, n_z, half, width), BF16),
            dma((6,)),
            dma((1,)),
            dma((REACH,)),
            dma((REACH,)),
            dma((4, 2)),
            dma((4, 2, 2)),
            dma((4, 2, 2)),
            dma((2,)),
            dma((2,)),
            dma((2, n_z // 2 - 2, 2, 2)),
            dma((2, n_z // 2 - 2, 2, 2)),
            dma((2, 2)),
            dma((2, 2, n_z)),
            dma((REACH,)),
            dma((REACH,)),
            dma((1, n_z - 1)),
            dma((1, n_z)),
            dma((2, 1)),
            dma((2, 2)),
            dma((2, SIDE - 1)),
            dma((2, SIDE)),
            dma((2, SIDE - 1)),
            dma((2, SIDE)),
            dma((1, n_z - 1)),
            dma((1, n_z)),
        ],
        compiler_params=pltpu.CompilerParams(collective_id=0, has_side_effects=True),
        name="fused",
    )(queries, keys, values, codes, wq_t, wkey_t)


def publish_kernel(*refs):
    half = len(refs) // 2
    for given, out in zip(refs[:half], refs[half:]):
        out[...] = given[...]


def publish(*results):
    return pl.pallas_call(
        publish_kernel,
        out_shape=tuple(jax.ShapeDtypeStruct(r.shape, r.dtype) for r in results),
        in_specs=[pl.BlockSpec(memory_space=VMEM)] * len(results),
        out_specs=(pl.BlockSpec(memory_space=VMEM),) * len(results),
        name="publish",
    )(*results)


def solution(mesh):
    n_seq, n_z = mesh.shape["seq"], mesh.shape["tensor"]

    def shards(queries, keys, values, doc_ids, w_query, w_key):
        count, width = keys.shape
        student, gwq, gwk, kfg = publish(
            *fused(
                queries.reshape(count, width),
                keys,
                values,
                doc_ids.reshape(1, count),
                w_query[0].T,
                w_key.T,
                n_seq,
                n_z,
            )
        )
        return student.reshape(queries.shape), gwq.T[None], gwk.T, kfg.T

    return jax.shard_map(
        shards,
        mesh=mesh,
        in_specs=(
            P("seq", "tensor", None),
            P("seq", None),
            P("seq", None),
            P("seq"),
            P("tensor", None, None),
            P(),
        ),
        out_specs=(P("seq", "tensor", None), P("tensor", None, None), P(), P("seq", "tensor")),
        check_vma=False,
    )
```

```python
import functools

import jax
import jax.numpy as jnp
from jax import lax
from jax.experimental import pallas as pl
from jax.experimental.pallas import tpu as pltpu
from jax.sharding import PartitionSpec as P

F32 = jnp.float32
BF16 = jnp.bfloat16
MESH = pl.DeviceIdType.MESH
VMEM = pltpu.VMEM

REACH = 4
SIDE = 4
NEGATIVE = -1e30
LOG2E = 1.4426950408889634
TILE = 256
ADJ_ROWS = 144


def dot(a, b, ca, cb):
    return lax.dot_general(a, b, (((ca,), (cb,)), ((), ())), preferred_element_type=F32)


def remote(src, dst, send_sem, recv_sem, **where):
    return pltpu.make_async_remote_copy(
        src_ref=src,
        dst_ref=dst,
        send_sem=send_sem,
        recv_sem=recv_sem,
        device_id=where,
        device_id_type=MESH,
    )


def signal(sem, **where):
    pl.semaphore_signal(sem, inc=1, device_id=where, device_id_type=MESH)


def features(rows, weights_t):
    logits = dot(weights_t, rows, 1, 1)
    up = jnp.exp(logits - jnp.max(logits, axis=0, keepdims=True))
    down = jnp.exp(jnp.min(logits, axis=0, keepdims=True) - logits)
    up = up / jnp.sum(up, axis=0, keepdims=True)
    down = down / jnp.sum(down, axis=0, keepdims=True)
    return jnp.concatenate([up, down], axis=0)


def features_back(feat, grad):
    half = feat.shape[0] // 2
    p, m, a, b = feat[:half], feat[half:], grad[:half], grad[half:]
    upper = p * (a - jnp.sum(a * p, axis=0, keepdims=True))
    lower = m * (b - jnp.sum(b * m, axis=0, keepdims=True))
    return upper - lower


def transposed(x):
    return x.astype(F32).T.astype(x.dtype)


def lane_copies(row, count):
    return jnp.broadcast_to(row, (count, row.shape[1])).T


def across(column, width):
    return jnp.concatenate([column] * (width // column.shape[1]), axis=1)


def fused_kernel(
    n_seq,
    n_z,
    q_hbm,
    k_hbm,
    v_hbm,
    c_hbm,
    wq_hbm,
    wkey_hbm,
    student_hbm,
    gwq_out,
    gwk_out,
    kfg_out,
    q_ref,
    k_ref,
    v_ref,
    c_ref,
    wq_ref,
    wkey_ref,
    student_ref,
    wk_ref,
    wv_ref,
    wc_ref,
    kcol_ref,
    fkf_ref,
    vt_ref,
    kfb_ref,
    kf_ref,
    qf_ref,
    top_ref,
    den_ref,
    acc_ref,
    num_ref,
    state_ref,
    ssum_ref,
    gqf_ref,
    gkf_ref,
    adj_ref,
    adj_in,
    spread_ref,
    gather_ref,
    core_ref,
    y_ref,
    x_ref,
    z_ref,
    load_sem,
    store_sem,
    code_send,
    code_recv,
    slice_send,
    slice_recv,
    pass_send,
    own_send,
    own_recv,
    ring_send,
    ring_recv,
    pair_send,
    pair_recv,
    adj_send,
    adj_recv,
    spread_send,
    spread_recv,
    core_send,
    core_recv,
    y_send,
    y_recv,
    x_send,
    x_recv,
    z_send,
    z_recv,
):
    count, width = k_ref.shape
    half = wkey_hbm.shape[0]
    total = float(count * n_seq)
    grad_scale = 2.0 / total
    factor = width**-0.5 * LOG2E
    s = lax.axis_index("seq")
    z = lax.axis_index("tensor")
    core = lax.rem(s, 2)
    partner = s + 1 - 2 * core
    y = lax.rem(s // 2, SIDE)
    x = s // (2 * SIDE)
    part = count // n_z
    share = 2 * half // n_z

    def later(d):
        return lax.rem(s + d, n_seq)

    def turn(d):
        return lax.rem(z + d + n_z, n_z)

    def along_y(i):
        return lax.rem(y + i, SIDE)

    def along_x(i):
        return lax.rem(x + i, SIDE)

    def seq_of(at_x, at_y):
        return (at_x * SIDE + at_y) * 2 + core

    def rows(p):
        return pl.ds(pl.multiple_of(p * part, part), part)

    loads = [
        pltpu.make_async_copy(far, near, load_sem.at[i])
        for i, (far, near) in enumerate(
            (
                (k_hbm, k_ref),
                (v_hbm, v_ref),
                (c_hbm, c_ref),
                (q_hbm, q_ref),
                (wq_hbm, wq_ref),
                (wkey_hbm, wkey_ref),
            )
        )
    ]
    for load in loads:
        load.start()

    barrier = pltpu.get_barrier_semaphore()
    for d in range(1, REACH + 1):
        signal(barrier, seq=later(n_seq - d))
        signal(barrier, seq=later(d))
    signal(barrier, seq=partner)
    for i in range(1, SIDE):
        signal(barrier, seq=seq_of(x, along_y(i)))
        signal(barrier, seq=seq_of(along_x(i), y))
    for i in range(1, n_z):
        signal(barrier, tensor=turn(i))
    for load in loads[:3]:
        load.wait()
    pl.semaphore_wait(barrier, 2 * REACH + 1 + 2 * (SIDE - 1) + n_z - 1)

    started = []

    def send(*args, **where):
        copy = remote(*args, **where)
        copy.start()
        started.append(copy)

    def arrive(here, send_sem, recv_sem):
        remote(here, here, send_sem, recv_sem, seq=partner).wait_recv()

    pairs = ((k_ref, wk_ref), (v_ref, wv_ref))
    last = n_z // 2
    direct = (z, turn(last), turn(last - 1), turn(1 - last))

    def send_slice(j, at):
        for kv, (own, window) in enumerate(pairs):
            remote(
                own.at[rows(direct[j])],
                window.at[2 - at, rows(direct[j])],
                slice_send.at[j, kv],
                slice_recv.at[j, at, kv],
                seq=later(3 - at),
            ).start()

    for j in range(2):
        send_slice(j, core)
    for d in range(1, REACH + 1):
        send(c_ref, wc_ref.at[d - 1], code_send.at[d - 1], code_recv.at[d - 1], seq=later(d))

    @pl.when(core == 0)
    def _():
        for kv, (own, window) in enumerate(pairs):
            remote(own, window.at[0], own_send.at[kv], own_recv.at[kv], seq=partner).start()

    def pass_to_partner(at, i, kv, piece, order):
        if at == 0 and i == 0:
            return
        window = pairs[kv][1]
        remote(
            window.at[3 - at - i, rows(piece)],
            window.at[3 if at == 0 else 1 - i, rows(piece)],
            pair_send.at[i, kv],
            pair_recv.at[i, kv, order],
            seq=partner,
        ).start()

    def from_partner(at, *orders):
        for order in orders:
            here = rows(turn(order_turn[order]))
            for kv in range(2):
                for i in range(at, 2):
                    arrive(pairs[kv][1].at[0, here], pair_send.at[i, kv], pair_recv.at[i, kv, order])

    order_turn = (0, -1, 1, -2, 2, -3, 3, last)

    def take_slice(at, j, order):
        for i in range(2):
            for kv in range(2):
                window = pairs[kv][1]
                here = window.at[3 - at - i, rows(direct[j])]
                arrive(here, slice_send.at[j, kv], slice_recv.at[j, i, kv])
                if j == 0:
                    for way in range(2):
                        ring_copy(at, way, 1, i, kv)
                if at == 1:
                    remote(
                        here,
                        window.at[3 - i, rows(direct[j])],
                        pass_send.at[j, i, kv],
                        slice_recv.at[j, i, kv],
                        seq=later(1),
                    ).start()
                pass_to_partner(at, i, kv, direct[j], order)

    def ring_copy(at, way, step, i, kv):
        piece = rows(turn(1 - step) if way == 0 else turn(step - 1))
        here = pairs[kv][1].at[3 - at - i, piece]
        remote(
            here,
            here,
            ring_send.at[way, step - 1, i, kv],
            ring_recv.at[way, step - 1, i, kv],
            tensor=turn(1 if way == 0 else -1),
        ).start()

    def ring_step(at, step):
        for i in range(2):
            for kv in range(2):
                for way in range(2):
                    piece = turn(-step) if way == 0 else turn(step)
                    here = pairs[kv][1].at[3 - at - i, rows(piece)]
                    arrive(here, ring_send.at[way, step - 1, i, kv], ring_recv.at[way, step - 1, i, kv])
                    if step < last - 2:
                        ring_copy(at, way, step + 1, i, kv)
                    pass_to_partner(at, i, kv, piece, 2 * step - 1 + way)

    for load in loads[3:]:
        load.wait()
    code = c_ref[...].astype(F32)
    leading = code[:, :1]
    lead = (code == leading).astype(F32)
    wkey_t = wkey_ref[...]
    kf = features(k_ref[...], wkey_t)
    kf_ref[...] = kf
    kft = kf.astype(BF16)
    kfb_ref[...] = kf.T.astype(BF16)
    qf = features(q_ref[...], wq_ref[...])
    qf_ref[...] = qf
    qft = qf.astype(BF16)
    vt_ref[:width] = transposed(v_ref[...])
    one = lax.broadcasted_iota(jnp.int32, (ADJ_ROWS - width, count), 0) == 0
    vt_ref[width:] = one.astype(F32).astype(BF16)
    kcol_ref[...] = lane_copies(code, width)

    def own_mask(start, limit):
        same = across(kcol_ref[:limit], TILE) == code[:, start:limit]
        key_at = lax.broadcasted_iota(jnp.int32, (limit, TILE), 0)
        query_at = lax.broadcasted_iota(jnp.int32, (limit, TILE), 1) + start
        return same & (key_at <= query_at)

    unit = (lax.broadcasted_iota(jnp.int32, (count, width), 1) == 0).astype(F32).astype(BF16)

    def own_tile(start):
        limit = start + TILE
        cols = slice(start, limit)
        same = across(kcol_ref[cols], limit) == code[:, :limit]
        key_at = lax.broadcasted_iota(jnp.int32, (TILE, limit), 1)
        query_at = lax.broadcasted_iota(jnp.int32, (TILE, limit), 0) + start
        scores = dot(q_ref[cols], k_ref[:limit], 1, 1)
        scores = jnp.where(same & (key_at <= query_at), scores * factor, NEGATIVE)
        top = jnp.broadcast_to(jnp.max(scores, axis=1, keepdims=True), (TILE, width))
        weights = jnp.exp2(scores - across(top, limit)).astype(BF16)
        top_ref[cols] = top
        acc_ref[cols] = dot(weights, jnp.concatenate([v_ref[:limit], unit[:limit]], axis=1), 1, 0)
        products = jnp.where(own_mask(start, limit), dot(kfb_ref[:limit], qft[:, cols], 1, 0), 0.0)
        den_ref[:, cols] = jnp.sum(products, axis=0, keepdims=True)
        num_ref[:, cols] = dot(vt_ref[:width, :limit], products.astype(BF16), 1, 0)

    def far_pieces(blocks, *orders):
        places = [(d, rows(turn(order_turn[n]))) for d in blocks for n in orders]
        keys = jnp.concatenate([wk_ref[d, r] for d, r in places], axis=0)
        vals = jnp.concatenate([wv_ref[d, r] for d, r in places], axis=0)
        codes = jnp.concatenate([wc_ref[d, :, r] for d, r in places], axis=1).astype(F32)
        size = keys.shape[0]
        feat = features(keys, wkey_t)
        for n, (d, r) in enumerate(places):
            fkf_ref[d, :, r] = feat[:, n * part : (n + 1) * part]
        chosen = feat.astype(BF16).astype(F32) * (codes == leading).astype(F32)
        state_ref[...] += dot(chosen.astype(BF16), vals, 1, 0)
        ssum_ref[...] += jnp.broadcast_to(jnp.sum(chosen, axis=1, keepdims=True), ssum_ref.shape)
        wide = jnp.concatenate([vals, unit[:size]], axis=1)
        for start in range(0, count, TILE):
            cols = slice(start, start + TILE)
            scores = dot(q_ref[cols], keys, 1, 1)
            same = across(kcol_ref[cols], size) == codes
            scores = jnp.where(same, scores * factor, NEGATIVE)
            old = top_ref[cols]
            top = jnp.maximum(old, jnp.max(scores, axis=1, keepdims=True))
            weights = jnp.exp2(scores - across(top, size)).astype(BF16)
            shrink = jnp.exp2(old - top)
            top_ref[cols] = top
            acc_ref[cols] = acc_ref[cols] * across(shrink, 2 * width) + dot(weights, wide, 1, 0)

    def own_tiles(first, end):
        for start in range(first, end, TILE):
            own_tile(start)

    def codes_arrive():
        for d in range(REACH):
            arrive(wc_ref.at[d], code_send.at[d], code_recv.at[d])

    state_ref[...] = jnp.zeros_like(state_ref)
    ssum_ref[...] = jnp.zeros_like(ssum_ref)

    @pl.when(core == 1)
    def _():
        own_tiles(0, count // 2)
        take_slice(1, 0, 0)
        send_slice(2, 1)
        own_tiles(count // 2, count)
        take_slice(1, 1, 7)
        send_slice(3, 1)
        codes_arrive()
        for kv in range(2):
            arrive(pairs[kv][1].at[0], own_send.at[kv], own_recv.at[kv])
        ring_step(1, 1)
        far_pieces((0,), 0, 1, 2, 3)
        take_slice(1, 2, 6)
        far_pieces((1, 2), 0, 1, 2, 7)
        ring_step(1, 2)
        take_slice(1, 3, 5)
        far_pieces((0,), 4, 5, 6, 7)
        far_pieces((1, 2), 3, 4, 5, 6)
        from_partner(1, 0, 1, 2, 7)
        far_pieces((3,), 0, 1, 2, 7)
        from_partner(1, 3, 4, 5, 6)
        far_pieces((3,), 3, 4, 5, 6)

    @pl.when(core == 0)
    def _():
        own_tiles(0, count // 2)
        send_slice(2, 0)
        own_tiles(count // 2, count)
        send_slice(3, 0)
        codes_arrive()
        from_partner(0, 0, 7)
        take_slice(0, 0, 0)
        far_pieces((0, 1), 0, 7)
        take_slice(0, 1, 7)
        ring_step(0, 1)
        from_partner(0, 1, 2)
        far_pieces((0, 1), 1, 2)
        take_slice(0, 2, 6)
        far_pieces((2, 3), 0, 7)
        ring_step(0, 2)
        from_partner(0, 3, 4, 5, 6)
        far_pieces((2, 3), 1, 2)
        take_slice(0, 3, 5)
        far_pieces((0, 1), 3, 4, 5, 6)
        far_pieces((2, 3), 3, 4, 5, 6)

    state = state_ref[...]
    state_sum = ssum_ref[:, :1]
    acc = acc_ref[...]
    teacher = (acc[:, :width] / acc[:, width : width + 1]).T
    numerator = num_ref[...] + lead * dot(state.T.astype(BF16), qft, 1, 0)
    denominator = den_ref[...] + lead * jnp.sum(
        qft.astype(F32) * state_sum, axis=0, keepdims=True
    )
    estimate = numerator / denominator
    grad_out = grad_scale * (estimate - teacher)
    grad_num = grad_out / denominator
    grad_den = -jnp.sum(grad_out * estimate, axis=0, keepdims=True) / denominator
    gnt = grad_num.astype(BF16)

    row = lax.broadcasted_iota(jnp.int32, (ADJ_ROWS - width, count), 0)
    tail = jnp.where(row == 0, grad_den * lead, 0.0)
    masked = jnp.concatenate([grad_num * lead, tail], axis=0).astype(BF16)
    adjoint = dot(masked, qft, 1, 1)
    mark = lax.broadcasted_iota(jnp.int32, adjoint.shape, 0)
    adj_ref[...] = jnp.where(mark == width + 1, leading, adjoint).astype(BF16)
    for d in range(1, REACH + 1):
        send(
            adj_ref,
            adj_in.at[d - 1],
            adj_send.at[d - 1],
            adj_recv.at[d - 1],
            seq=later(n_seq - d),
        )

    gqf_ref[...] = lead * (dot(state.astype(BF16), gnt, 1, 0) + state_sum * grad_den)
    for start in range(0, count, TILE):
        limit = start + TILE
        cols = slice(start, limit)
        grad_prod = dot(v_ref[:limit], gnt[:, cols], 1, 0) + grad_den[:, cols]
        grad_prod = jnp.where(own_mask(start, limit), grad_prod, 0.0).astype(BF16)
        gqf_ref[:, cols] += dot(kft[:, :limit], grad_prod, 1, 0)
        piece = dot(qft[:, cols], grad_prod, 1, 1)
        if start:
            gkf_ref[:, :start] += piece[:, :start]
        gkf_ref[:, cols] = piece[:, start:]

    def wait(ref, which, at, send_sems, recv_sems):
        here = ref.at[which, at]
        arrive(here, send_sems.at[which, 0], recv_sems.at[which, at])

    def summed(ref, which):
        result = ref[which, 0].astype(F32)
        for i in range(1, ref.shape[1]):
            result = result + ref[which, i].astype(F32)
        return result

    def over_core(which, value):
        core_ref[which, core] = value.astype(BF16)
        here = core_ref.at[which, core]
        send(here, here, core_send.at[which, 0], core_recv.at[which, core], seq=partner)

    def over_y(which):
        wait(core_ref, which, 1 - core, core_send, core_recv)
        y_ref[which, y] = summed(core_ref, which).astype(BF16)
        here = y_ref.at[which, y]
        for i in range(1, SIDE):
            to = seq_of(x, along_y(i))
            send(here, here, y_send.at[which, i - 1], y_recv.at[which, y], seq=to)

    def over_x(which):
        for i in range(1, SIDE):
            wait(y_ref, which, along_y(i), y_send, y_recv)
        x_ref[which, x] = summed(y_ref, which).astype(BF16)
        here = x_ref.at[which, x]
        for i in range(1, SIDE):
            to = seq_of(along_x(i), y)
            send(here, here, x_send.at[which, i - 1], x_recv.at[which, x], seq=to)

    def over_seq(which):
        for i in range(1, SIDE):
            wait(x_ref, which, along_x(i), x_send, x_recv)
        return summed(x_ref, which)

    grad_ak = features_back(kf_ref[...], gkf_ref[...]).astype(BF16)
    grad_wk = dot(grad_ak, k_ref[...], 1, 0)
    adjoint_t = adjoint.T
    adjoint_b = adjoint_t[:, :width].astype(BF16)
    adjoint_sum = adjoint_t[:, width : width + 1]
    for d in range(REACH):
        met = (wc_ref[d].astype(F32) == leading).astype(F32)
        caused = (dot(adjoint_b, wv_ref[d], 1, 1) + adjoint_sum) * met
        grad_ak = features_back(fkf_ref[d], caused).astype(BF16)
        grad_wk = grad_wk + dot(grad_ak, wk_ref[d], 1, 0)
    over_core(1, grad_wk)

    grad_aq = features_back(qf_ref[...], gqf_ref[...]).astype(BF16)
    over_core(0, dot(grad_aq, q_ref[...], 1, 0))
    student_ref[...] = estimate.T.astype(BF16)
    store = pltpu.make_async_copy(student_ref, student_hbm, store_sem.at[0])
    store.start()
    over_y(1)

    final = code[:, count - 1 :]
    back = (code == final).astype(F32)
    entering = jnp.zeros(adj_ref.shape, F32)
    for d in range(REACH):
        arrive(adj_in.at[d], adj_send.at[d], adj_recv.at[d])
        arrived = adj_in[d].astype(F32)
        entering = entering + jnp.where(arrived[width + 1 : width + 2] == final, arrived, 0.0)
    added = dot(entering.T.astype(BF16), vt_ref[...], 1, 0)
    grad_kf = gkf_ref[...] + back * added
    spread_ref[...] = (grad_kf * total).astype(BF16)
    for i in range(1, n_z):
        to = turn(i)
        send(
            spread_ref.at[pl.ds(pl.multiple_of(to * share, share), share)],
            gather_ref.at[0, z],
            spread_send.at[0, i - 1],
            spread_recv.at[0, z],
            tensor=to,
        )
    gather_ref[0, z] = spread_ref[pl.ds(pl.multiple_of(z * share, share), share)]

    over_x(1)
    over_y(0)
    z_ref[0, z] = over_seq(1).astype(BF16)
    here = z_ref.at[0, z]
    for i in range(1, n_z):
        send(here, here, z_send.at[0, i - 1], z_recv.at[0, z], tensor=turn(i))
    over_x(0)
    gwq_out[...] = over_seq(0)
    for i in range(1, n_z):
        wait(gather_ref, 0, turn(i), spread_send, spread_recv)
    kfg_out[...] = summed(gather_ref, 0)
    for i in range(1, n_z):
        wait(z_ref, 0, turn(i), z_send, z_recv)
    gwk_out[...] = summed(z_ref, 0)

    store.wait()
    for copy in started:
        copy.wait_send()
    for kv, (own, window) in enumerate(pairs):
        block = window.at[0]
        here = window.at[0, rows(z)]
        for j in range(len(direct)):
            remote(here, here, slice_send.at[j, kv], own_recv.at[kv], seq=partner).wait_send()
        for way in range(2):
            for step in range(last - 2):
                for i in range(2):
                    remote(
                        here, here, ring_send.at[way, step, i, kv], own_recv.at[kv], seq=partner
                    ).wait_send()
        remote(block, block, pair_send.at[1, kv], own_recv.at[kv], seq=partner).wait_send()

        @pl.when(core == 1)
        def _():
            remote(block, block, pair_send.at[0, kv], own_recv.at[kv], seq=partner).wait_send()
            for j in range(len(direct)):
                for i in range(2):
                    remote(here, here, pass_send.at[j, i, kv], own_recv.at[kv], seq=partner).wait_send()

        @pl.when(core == 0)
        def _():
            remote(own, block, own_send.at[kv], own_recv.at[kv], seq=partner).wait_send()


def fused(queries, keys, values, codes, wq_t, wkey_t, n_seq, n_z):
    count, width = keys.shape
    half = wkey_t.shape[0]
    feat = 2 * half
    dma = pltpu.SemaphoreType.DMA
    return pl.pallas_call(
        functools.partial(fused_kernel, n_seq, n_z),
        out_shape=(
            jax.ShapeDtypeStruct((count, width), BF16),
            jax.ShapeDtypeStruct((half, width), F32),
            jax.ShapeDtypeStruct((half, width), F32),
            jax.ShapeDtypeStruct((feat // n_z, count), F32),
        ),
        in_specs=[pl.BlockSpec(memory_space=pl.ANY)] * 6,
        out_specs=(
            pl.BlockSpec(memory_space=pl.ANY),
            *[pl.BlockSpec(memory_space=VMEM)] * 3,
        ),
        scratch_shapes=[
            VMEM((count, width), BF16),
            VMEM((count, width), BF16),
            VMEM((count, width), BF16),
            VMEM((1, count), jnp.int32),
            VMEM((half, width), BF16),
            VMEM((half, width), BF16),
            VMEM((count, width), BF16),
            VMEM((REACH, count, width), BF16),
            VMEM((REACH, count, width), BF16),
            VMEM((REACH, 1, count), jnp.int32),
            VMEM((count, width), F32),
            VMEM((REACH, feat, count), F32),
            VMEM((ADJ_ROWS, count), BF16),
            VMEM((count, feat), BF16),
            VMEM((feat, count), F32),
            VMEM((feat, count), F32),
            VMEM((count, width), F32),
            VMEM((1, count), F32),
            VMEM((count, 2 * width), F32),
            VMEM((width, count), F32),
            VMEM((feat, width), F32),
            VMEM((feat, width), F32),
            VMEM((feat, count), F32),
            VMEM((feat, count), F32),
            VMEM((ADJ_ROWS, feat), BF16),
            VMEM((REACH, ADJ_ROWS, feat), BF16),
            VMEM((feat, count), BF16),
            VMEM((1, n_z, feat // n_z, count), BF16),
            VMEM((2, 2, half, width), BF16),
            VMEM((2, SIDE, half, width), BF16),
            VMEM((2, SIDE, half, width), BF16),
            VMEM((1, n_z, half, width), BF16),
            dma((6,)),
            dma((1,)),
            dma((REACH,)),
            dma((REACH,)),
            dma((4, 2)),
            dma((4, 2, 2)),
            dma((4, 2, 2)),
            dma((2,)),
            dma((2,)),
            dma((2, n_z // 2 - 2, 2, 2)),
            dma((2, n_z // 2 - 2, 2, 2)),
            dma((2, 2)),
            dma((2, 2, n_z)),
            dma((REACH,)),
            dma((REACH,)),
            dma((1, n_z - 1)),
            dma((1, n_z)),
            dma((2, 1)),
            dma((2, 2)),
            dma((2, SIDE - 1)),
            dma((2, SIDE)),
            dma((2, SIDE - 1)),
            dma((2, SIDE)),
            dma((1, n_z - 1)),
            dma((1, n_z)),
        ],
        compiler_params=pltpu.CompilerParams(collective_id=0, has_side_effects=True),
        name="fused",
    )(queries, keys, values, codes, wq_t, wkey_t)


def publish_kernel(*refs):
    half = len(refs) // 2
    for given, out in zip(refs[:half], refs[half:]):
        out[...] = given[...]


def publish(*results):
    return pl.pallas_call(
        publish_kernel,
        out_shape=tuple(jax.ShapeDtypeStruct(r.shape, r.dtype) for r in results),
        in_specs=[pl.BlockSpec(memory_space=VMEM)] * len(results),
        out_specs=(pl.BlockSpec(memory_space=VMEM),) * len(results),
        name="publish",
    )(*results)


def solution(mesh):
    n_seq, n_z = mesh.shape["seq"], mesh.shape["tensor"]

    def shards(queries, keys, values, doc_ids, w_query, w_key):
        count, width = keys.shape
        student, gwq, gwk, kfg = publish(
            *fused(
                queries.reshape(count, width),
                keys,
                values,
                doc_ids.reshape(1, count),
                w_query[0].T,
                w_key.T,
                n_seq,
                n_z,
            )
        )
        return student.reshape(queries.shape), gwq.T[None], gwk.T, kfg.T

    return jax.shard_map(
        shards,
        mesh=mesh,
        in_specs=(
            P("seq", "tensor", None),
            P("seq", None),
            P("seq", None),
            P("seq"),
            P("tensor", None, None),
            P(),
        ),
        out_specs=(P("seq", "tensor", None), P("tensor", None, None), P(), P("seq", "tensor")),
        check_vma=False,
    )
```

```python
import functools

import jax
import jax.numpy as jnp
from jax import lax
from jax.experimental import pallas as pl
from jax.experimental.pallas import tpu as pltpu
from jax.sharding import PartitionSpec as P

F32 = jnp.float32
BF16 = jnp.bfloat16
MESH = pl.DeviceIdType.MESH
VMEM = pltpu.VMEM

REACH = 4
SIDE = 4
NEGATIVE = -1e30
LOG2E = 1.4426950408889634
TILE = 256
ADJ_ROWS = 144


def dot(a, b, ca, cb):
    return lax.dot_general(a, b, (((ca,), (cb,)), ((), ())), preferred_element_type=F32)


def remote(src, dst, send_sem, recv_sem, **where):
    return pltpu.make_async_remote_copy(
        src_ref=src,
        dst_ref=dst,
        send_sem=send_sem,
        recv_sem=recv_sem,
        device_id=where,
        device_id_type=MESH,
    )


def signal(sem, **where):
    pl.semaphore_signal(sem, inc=1, device_id=where, device_id_type=MESH)


def features(rows, weights_t):
    logits = dot(weights_t, rows, 1, 1)
    up = jnp.exp(logits - jnp.max(logits, axis=0, keepdims=True))
    down = jnp.exp(jnp.min(logits, axis=0, keepdims=True) - logits)
    up = up / jnp.sum(up, axis=0, keepdims=True)
    down = down / jnp.sum(down, axis=0, keepdims=True)
    return jnp.concatenate([up, down], axis=0)


def features_back(feat, grad):
    half = feat.shape[0] // 2
    p, m, a, b = feat[:half], feat[half:], grad[:half], grad[half:]
    upper = p * (a - jnp.sum(a * p, axis=0, keepdims=True))
    lower = m * (b - jnp.sum(b * m, axis=0, keepdims=True))
    return upper - lower


def transposed(x):
    return x.astype(F32).T.astype(x.dtype)


def lane_copies(row, count):
    return jnp.broadcast_to(row, (count, row.shape[1])).T


def across(column, width):
    return jnp.concatenate([column] * (width // column.shape[1]), axis=1)


def fused_kernel(
    n_seq,
    n_z,
    q_hbm,
    k_hbm,
    v_hbm,
    c_hbm,
    wq_hbm,
    wkey_hbm,
    student_hbm,
    gwq_out,
    gwk_out,
    kfg_out,
    q_ref,
    k_ref,
    v_ref,
    c_ref,
    wq_ref,
    wkey_ref,
    student_ref,
    wk_ref,
    wv_ref,
    wc_ref,
    kcol_ref,
    fkf_ref,
    vt_ref,
    kfb_ref,
    kf_ref,
    qf_ref,
    top_ref,
    den_ref,
    acc_ref,
    num_ref,
    state_ref,
    ssum_ref,
    gqf_ref,
    gkf_ref,
    adj_ref,
    adj_in,
    spread_ref,
    gather_ref,
    row_ref,
    x_ref,
    z_ref,
    load_sem,
    store_sem,
    code_send,
    code_recv,
    slice_send,
    slice_recv,
    pass_send,
    own_send,
    own_recv,
    ring_send,
    ring_recv,
    pair_send,
    pair_recv,
    adj_send,
    adj_recv,
    spread_send,
    spread_recv,
    row_send,
    row_recv,
    x_send,
    x_recv,
    z_send,
    z_recv,
):
    count, width = k_ref.shape
    half = wkey_hbm.shape[0]
    total = float(count * n_seq)
    grad_scale = 2.0 / total
    factor = width**-0.5 * LOG2E
    s = lax.axis_index("seq")
    z = lax.axis_index("tensor")
    core = lax.rem(s, 2)
    partner = s + 1 - 2 * core
    row = 2 * SIDE
    at_row = lax.rem(s, row)
    x = s // row
    part = count // n_z
    share = 2 * half // n_z

    def later(d):
        return lax.rem(s + d, n_seq)

    def turn(d):
        return lax.rem(z + d + n_z, n_z)

    def along_row(i):
        return lax.rem(at_row + i, row)

    def along_x(i):
        return lax.rem(x + i, SIDE)

    def seq_of(to_x, to_row):
        return to_x * row + to_row

    def rows(p):
        return pl.ds(pl.multiple_of(p * part, part), part)

    loads = [
        pltpu.make_async_copy(far, near, load_sem.at[i])
        for i, (far, near) in enumerate(
            (
                (k_hbm, k_ref),
                (v_hbm, v_ref),
                (c_hbm, c_ref),
                (q_hbm, q_ref),
                (wq_hbm, wq_ref),
                (wkey_hbm, wkey_ref),
            )
        )
    ]
    for load in loads:
        load.start()

    barrier = pltpu.get_barrier_semaphore()
    for d in range(1, REACH + 1):
        signal(barrier, seq=later(n_seq - d))
        signal(barrier, seq=later(d))
    for i in range(1, row):
        signal(barrier, seq=seq_of(x, along_row(i)))
    for i in range(1, SIDE):
        signal(barrier, seq=seq_of(along_x(i), at_row))
    for i in range(1, n_z):
        signal(barrier, tensor=turn(i))
    for load in loads[:3]:
        load.wait()
    pl.semaphore_wait(barrier, 2 * REACH + row - 1 + SIDE - 1 + n_z - 1)

    started = []

    def send(*args, **where):
        copy = remote(*args, **where)
        copy.start()
        started.append(copy)

    def arrive(here, send_sem, recv_sem):
        remote(here, here, send_sem, recv_sem, seq=partner).wait_recv()

    pairs = ((k_ref, wk_ref), (v_ref, wv_ref))
    last = n_z // 2
    direct = (z, turn(last), turn(last - 1), turn(1 - last))

    def send_slice(j, at):
        for kv, (own, window) in enumerate(pairs):
            remote(
                own.at[rows(direct[j])],
                window.at[2 - at, rows(direct[j])],
                slice_send.at[j, kv],
                slice_recv.at[j, at, kv],
                seq=later(3 - at),
            ).start()

    for j in range(2):
        send_slice(j, core)
    for d in range(1, REACH + 1):
        send(c_ref, wc_ref.at[d - 1], code_send.at[d - 1], code_recv.at[d - 1], seq=later(d))

    @pl.when(core == 0)
    def _():
        for kv, (own, window) in enumerate(pairs):
            remote(own, window.at[0], own_send.at[kv], own_recv.at[kv], seq=partner).start()

    def pass_to_partner(at, i, kv, piece, order):
        if at == 0 and i == 0:
            return
        window = pairs[kv][1]
        remote(
            window.at[3 - at - i, rows(piece)],
            window.at[3 if at == 0 else 1 - i, rows(piece)],
            pair_send.at[i, kv],
            pair_recv.at[i, kv, order],
            seq=partner,
        ).start()

    def from_partner(at, *orders):
        for order in orders:
            here = rows(turn(order_turn[order]))
            for kv in range(2):
                for i in range(at, 2):
                    arrive(pairs[kv][1].at[0, here], pair_send.at[i, kv], pair_recv.at[i, kv, order])

    order_turn = (0, -1, 1, -2, 2, -3, 3, last)

    def take_slice(at, j, order):
        for i in range(2):
            for kv in range(2):
                window = pairs[kv][1]
                here = window.at[3 - at - i, rows(direct[j])]
                arrive(here, slice_send.at[j, kv], slice_recv.at[j, i, kv])
                if j == 0:
                    for way in range(2):
                        ring_copy(at, way, 1, i, kv)
                if at == 1:
                    remote(
                        here,
                        window.at[3 - i, rows(direct[j])],
                        pass_send.at[j, i, kv],
                        slice_recv.at[j, i, kv],
                        seq=later(1),
                    ).start()
                pass_to_partner(at, i, kv, direct[j], order)

    def ring_copy(at, way, step, i, kv):
        piece = rows(turn(1 - step) if way == 0 else turn(step - 1))
        here = pairs[kv][1].at[3 - at - i, piece]
        remote(
            here,
            here,
            ring_send.at[way, step - 1, i, kv],
            ring_recv.at[way, step - 1, i, kv],
            tensor=turn(1 if way == 0 else -1),
        ).start()

    def ring_step(at, step):
        for i in range(2):
            for kv in range(2):
                for way in range(2):
                    piece = turn(-step) if way == 0 else turn(step)
                    here = pairs[kv][1].at[3 - at - i, rows(piece)]
                    arrive(here, ring_send.at[way, step - 1, i, kv], ring_recv.at[way, step - 1, i, kv])
                    if step < last - 2:
                        ring_copy(at, way, step + 1, i, kv)
                    pass_to_partner(at, i, kv, piece, 2 * step - 1 + way)

    for load in loads[3:]:
        load.wait()
    code = c_ref[...].astype(F32)
    leading = code[:, :1]
    lead = (code == leading).astype(F32)
    wkey_t = wkey_ref[...]
    kf = features(k_ref[...], wkey_t)
    kf_ref[...] = kf
    kft = kf.astype(BF16)
    kfb_ref[...] = kf.T.astype(BF16)
    qf = features(q_ref[...], wq_ref[...])
    qf_ref[...] = qf
    qft = qf.astype(BF16)
    vt_ref[:width] = transposed(v_ref[...])
    one = lax.broadcasted_iota(jnp.int32, (ADJ_ROWS - width, count), 0) == 0
    vt_ref[width:] = one.astype(F32).astype(BF16)
    kcol_ref[...] = lane_copies(code, width)

    def own_mask(start, limit):
        same = across(kcol_ref[:limit], TILE) == code[:, start:limit]
        key_at = lax.broadcasted_iota(jnp.int32, (limit, TILE), 0)
        query_at = lax.broadcasted_iota(jnp.int32, (limit, TILE), 1) + start
        return same & (key_at <= query_at)

    unit = (lax.broadcasted_iota(jnp.int32, (count, width), 1) == 0).astype(F32).astype(BF16)

    def own_tile(start):
        limit = start + TILE
        cols = slice(start, limit)
        same = across(kcol_ref[cols], limit) == code[:, :limit]
        key_at = lax.broadcasted_iota(jnp.int32, (TILE, limit), 1)
        query_at = lax.broadcasted_iota(jnp.int32, (TILE, limit), 0) + start
        scores = dot(q_ref[cols], k_ref[:limit], 1, 1)
        scores = jnp.where(same & (key_at <= query_at), scores * factor, NEGATIVE)
        top = jnp.broadcast_to(jnp.max(scores, axis=1, keepdims=True), (TILE, width))
        weights = jnp.exp2(scores - across(top, limit)).astype(BF16)
        top_ref[cols] = top
        acc_ref[cols] = dot(weights, jnp.concatenate([v_ref[:limit], unit[:limit]], axis=1), 1, 0)
        products = jnp.where(own_mask(start, limit), dot(kfb_ref[:limit], qft[:, cols], 1, 0), 0.0)
        den_ref[:, cols] = jnp.sum(products, axis=0, keepdims=True)
        num_ref[:, cols] = dot(vt_ref[:width, :limit], products.astype(BF16), 1, 0)

    def far_pieces(blocks, *orders):
        places = [(d, rows(turn(order_turn[n]))) for d in blocks for n in orders]
        keys = jnp.concatenate([wk_ref[d, r] for d, r in places], axis=0)
        vals = jnp.concatenate([wv_ref[d, r] for d, r in places], axis=0)
        codes = jnp.concatenate([wc_ref[d, :, r] for d, r in places], axis=1).astype(F32)
        size = keys.shape[0]
        feat = features(keys, wkey_t)
        for n, (d, r) in enumerate(places):
            fkf_ref[d, :, r] = feat[:, n * part : (n + 1) * part]
        chosen = feat.astype(BF16).astype(F32) * (codes == leading).astype(F32)
        state_ref[...] += dot(chosen.astype(BF16), vals, 1, 0)
        ssum_ref[...] += jnp.broadcast_to(jnp.sum(chosen, axis=1, keepdims=True), ssum_ref.shape)
        wide = jnp.concatenate([vals, unit[:size]], axis=1)
        for start in range(0, count, TILE):
            cols = slice(start, start + TILE)
            scores = dot(q_ref[cols], keys, 1, 1)
            same = across(kcol_ref[cols], size) == codes
            scores = jnp.where(same, scores * factor, NEGATIVE)
            old = top_ref[cols]
            top = jnp.maximum(old, jnp.max(scores, axis=1, keepdims=True))
            weights = jnp.exp2(scores - across(top, size)).astype(BF16)
            shrink = jnp.exp2(old - top)
            top_ref[cols] = top
            acc_ref[cols] = acc_ref[cols] * across(shrink, 2 * width) + dot(weights, wide, 1, 0)

    def own_tiles(first, end):
        for start in range(first, end, TILE):
            own_tile(start)

    def codes_arrive():
        for d in range(REACH):
            arrive(wc_ref.at[d], code_send.at[d], code_recv.at[d])

    state_ref[...] = jnp.zeros_like(state_ref)
    ssum_ref[...] = jnp.zeros_like(ssum_ref)

    @pl.when(core == 1)
    def _():
        own_tiles(0, count // 2)
        take_slice(1, 0, 0)
        send_slice(2, 1)
        own_tiles(count // 2, count)
        take_slice(1, 1, 7)
        send_slice(3, 1)
        codes_arrive()
        for kv in range(2):
            arrive(pairs[kv][1].at[0], own_send.at[kv], own_recv.at[kv])
        ring_step(1, 1)
        far_pieces((0,), 0, 1, 2, 3)
        take_slice(1, 2, 6)
        far_pieces((1, 2), 0, 1, 2, 7)
        ring_step(1, 2)
        take_slice(1, 3, 5)
        far_pieces((0,), 4, 5, 6, 7)
        far_pieces((1, 2), 3, 4, 5, 6)
        from_partner(1, 0, 1, 2, 7)
        far_pieces((3,), 0, 1, 2, 7)
        from_partner(1, 3, 4, 5, 6)
        far_pieces((3,), 3, 4, 5, 6)

    @pl.when(core == 0)
    def _():
        own_tiles(0, count // 2)
        send_slice(2, 0)
        own_tiles(count // 2, count)
        send_slice(3, 0)
        codes_arrive()
        from_partner(0, 0, 7)
        take_slice(0, 0, 0)
        far_pieces((0, 1), 0, 7)
        take_slice(0, 1, 7)
        ring_step(0, 1)
        from_partner(0, 1, 2)
        far_pieces((0, 1), 1, 2)
        take_slice(0, 2, 6)
        far_pieces((2, 3), 0, 7)
        ring_step(0, 2)
        from_partner(0, 3, 4, 5, 6)
        far_pieces((2, 3), 1, 2)
        take_slice(0, 3, 5)
        far_pieces((0, 1), 3, 4, 5, 6)
        far_pieces((2, 3), 3, 4, 5, 6)

    state = state_ref[...]
    state_sum = ssum_ref[:, :1]
    acc = acc_ref[...]
    teacher = (acc[:, :width] / acc[:, width : width + 1]).T
    numerator = num_ref[...] + lead * dot(state.T.astype(BF16), qft, 1, 0)
    denominator = den_ref[...] + lead * jnp.sum(
        qft.astype(F32) * state_sum, axis=0, keepdims=True
    )
    estimate = numerator / denominator
    grad_out = grad_scale * (estimate - teacher)
    grad_num = grad_out / denominator
    grad_den = -jnp.sum(grad_out * estimate, axis=0, keepdims=True) / denominator
    gnt = grad_num.astype(BF16)

    line = lax.broadcasted_iota(jnp.int32, (ADJ_ROWS - width, count), 0)
    tail = jnp.where(line == 0, grad_den * lead, 0.0)
    masked = jnp.concatenate([grad_num * lead, tail], axis=0).astype(BF16)
    adjoint = dot(masked, qft, 1, 1)
    mark = lax.broadcasted_iota(jnp.int32, adjoint.shape, 0)
    adj_ref[...] = jnp.where(mark == width + 1, leading, adjoint).astype(BF16)
    for d in range(1, REACH + 1):
        send(
            adj_ref,
            adj_in.at[d - 1],
            adj_send.at[d - 1],
            adj_recv.at[d - 1],
            seq=later(n_seq - d),
        )

    gqf_ref[...] = lead * (dot(state.astype(BF16), gnt, 1, 0) + state_sum * grad_den)
    for start in range(0, count, TILE):
        limit = start + TILE
        cols = slice(start, limit)
        grad_prod = dot(v_ref[:limit], gnt[:, cols], 1, 0) + grad_den[:, cols]
        grad_prod = jnp.where(own_mask(start, limit), grad_prod, 0.0).astype(BF16)
        gqf_ref[:, cols] += dot(kft[:, :limit], grad_prod, 1, 0)
        piece = dot(qft[:, cols], grad_prod, 1, 1)
        if start:
            gkf_ref[:, :start] += piece[:, :start]
        gkf_ref[:, cols] = piece[:, start:]

    def wait(ref, which, at, send_sems, recv_sems):
        here = ref.at[which, at]
        arrive(here, send_sems.at[which, 0], recv_sems.at[which, at])

    def summed(ref, which):
        result = ref[which, 0].astype(F32)
        for i in range(1, ref.shape[1]):
            result = result + ref[which, i].astype(F32)
        return result

    def over_row(which, value):
        row_ref[which, at_row] = value.astype(BF16)
        here = row_ref.at[which, at_row]
        for i in range(1, row):
            to = seq_of(x, along_row(i))
            send(here, here, row_send.at[which, i - 1], row_recv.at[which, at_row], seq=to)

    def over_x(which):
        for i in range(1, row):
            wait(row_ref, which, along_row(i), row_send, row_recv)
        x_ref[which, x] = summed(row_ref, which).astype(BF16)
        here = x_ref.at[which, x]
        for i in range(1, SIDE):
            to = seq_of(along_x(i), at_row)
            send(here, here, x_send.at[which, i - 1], x_recv.at[which, x], seq=to)

    def over_seq(which):
        for i in range(1, SIDE):
            wait(x_ref, which, along_x(i), x_send, x_recv)
        return summed(x_ref, which)

    grad_ak = features_back(kf_ref[...], gkf_ref[...]).astype(BF16)
    grad_wk = dot(grad_ak, k_ref[...], 1, 0)
    adjoint_t = adjoint.T
    adjoint_b = adjoint_t[:, :width].astype(BF16)
    adjoint_sum = adjoint_t[:, width : width + 1]
    for d in range(REACH):
        met = (wc_ref[d].astype(F32) == leading).astype(F32)
        caused = (dot(adjoint_b, wv_ref[d], 1, 1) + adjoint_sum) * met
        grad_ak = features_back(fkf_ref[d], caused).astype(BF16)
        grad_wk = grad_wk + dot(grad_ak, wk_ref[d], 1, 0)
    over_row(1, grad_wk)

    grad_aq = features_back(qf_ref[...], gqf_ref[...]).astype(BF16)
    over_row(0, dot(grad_aq, q_ref[...], 1, 0))
    student_ref[...] = estimate.T.astype(BF16)
    store = pltpu.make_async_copy(student_ref, student_hbm, store_sem.at[0])
    store.start()

    final = code[:, count - 1 :]
    back = (code == final).astype(F32)
    entering = jnp.zeros(adj_ref.shape, F32)
    for d in range(REACH):
        arrive(adj_in.at[d], adj_send.at[d], adj_recv.at[d])
        arrived = adj_in[d].astype(F32)
        entering = entering + jnp.where(arrived[width + 1 : width + 2] == final, arrived, 0.0)
    added = dot(entering.T.astype(BF16), vt_ref[...], 1, 0)
    grad_kf = gkf_ref[...] + back * added
    spread_ref[...] = (grad_kf * total).astype(BF16)
    for i in range(1, n_z):
        to = turn(i)
        send(
            spread_ref.at[pl.ds(pl.multiple_of(to * share, share), share)],
            gather_ref.at[0, z],
            spread_send.at[0, i - 1],
            spread_recv.at[0, z],
            tensor=to,
        )
    gather_ref[0, z] = spread_ref[pl.ds(pl.multiple_of(z * share, share), share)]

    over_x(1)
    z_ref[0, z] = over_seq(1).astype(BF16)
    here = z_ref.at[0, z]
    for i in range(1, n_z):
        send(here, here, z_send.at[0, i - 1], z_recv.at[0, z], tensor=turn(i))
    over_x(0)
    gwq_out[...] = over_seq(0)
    for i in range(1, n_z):
        wait(gather_ref, 0, turn(i), spread_send, spread_recv)
    kfg_out[...] = summed(gather_ref, 0)
    for i in range(1, n_z):
        wait(z_ref, 0, turn(i), z_send, z_recv)
    gwk_out[...] = summed(z_ref, 0)

    store.wait()
    for copy in started:
        copy.wait_send()
    for kv, (own, window) in enumerate(pairs):
        block = window.at[0]
        here = window.at[0, rows(z)]
        for j in range(len(direct)):
            remote(here, here, slice_send.at[j, kv], own_recv.at[kv], seq=partner).wait_send()
        for way in range(2):
            for step in range(last - 2):
                for i in range(2):
                    remote(
                        here, here, ring_send.at[way, step, i, kv], own_recv.at[kv], seq=partner
                    ).wait_send()
        remote(block, block, pair_send.at[1, kv], own_recv.at[kv], seq=partner).wait_send()

        @pl.when(core == 1)
        def _():
            remote(block, block, pair_send.at[0, kv], own_recv.at[kv], seq=partner).wait_send()
            for j in range(len(direct)):
                for i in range(2):
                    remote(here, here, pass_send.at[j, i, kv], own_recv.at[kv], seq=partner).wait_send()

        @pl.when(core == 0)
        def _():
            remote(own, block, own_send.at[kv], own_recv.at[kv], seq=partner).wait_send()


def fused(queries, keys, values, codes, wq_t, wkey_t, n_seq, n_z):
    count, width = keys.shape
    half = wkey_t.shape[0]
    feat = 2 * half
    dma = pltpu.SemaphoreType.DMA
    return pl.pallas_call(
        functools.partial(fused_kernel, n_seq, n_z),
        out_shape=(
            jax.ShapeDtypeStruct((count, width), BF16),
            jax.ShapeDtypeStruct((half, width), F32),
            jax.ShapeDtypeStruct((half, width), F32),
            jax.ShapeDtypeStruct((feat // n_z, count), F32),
        ),
        in_specs=[pl.BlockSpec(memory_space=pl.ANY)] * 6,
        out_specs=(
            pl.BlockSpec(memory_space=pl.ANY),
            *[pl.BlockSpec(memory_space=VMEM)] * 3,
        ),
        scratch_shapes=[
            VMEM((count, width), BF16),
            VMEM((count, width), BF16),
            VMEM((count, width), BF16),
            VMEM((1, count), jnp.int32),
            VMEM((half, width), BF16),
            VMEM((half, width), BF16),
            VMEM((count, width), BF16),
            VMEM((REACH, count, width), BF16),
            VMEM((REACH, count, width), BF16),
            VMEM((REACH, 1, count), jnp.int32),
            VMEM((count, width), F32),
            VMEM((REACH, feat, count), F32),
            VMEM((ADJ_ROWS, count), BF16),
            VMEM((count, feat), BF16),
            VMEM((feat, count), F32),
            VMEM((feat, count), F32),
            VMEM((count, width), F32),
            VMEM((1, count), F32),
            VMEM((count, 2 * width), F32),
            VMEM((width, count), F32),
            VMEM((feat, width), F32),
            VMEM((feat, width), F32),
            VMEM((feat, count), F32),
            VMEM((feat, count), F32),
            VMEM((ADJ_ROWS, feat), BF16),
            VMEM((REACH, ADJ_ROWS, feat), BF16),
            VMEM((feat, count), BF16),
            VMEM((1, n_z, feat // n_z, count), BF16),
            VMEM((2, 2 * SIDE, half, width), BF16),
            VMEM((2, SIDE, half, width), BF16),
            VMEM((1, n_z, half, width), BF16),
            dma((6,)),
            dma((1,)),
            dma((REACH,)),
            dma((REACH,)),
            dma((4, 2)),
            dma((4, 2, 2)),
            dma((4, 2, 2)),
            dma((2,)),
            dma((2,)),
            dma((2, n_z // 2 - 2, 2, 2)),
            dma((2, n_z // 2 - 2, 2, 2)),
            dma((2, 2)),
            dma((2, 2, n_z)),
            dma((REACH,)),
            dma((REACH,)),
            dma((1, n_z - 1)),
            dma((1, n_z)),
            dma((2, 2 * SIDE - 1)),
            dma((2, 2 * SIDE)),
            dma((2, SIDE - 1)),
            dma((2, SIDE)),
            dma((1, n_z - 1)),
            dma((1, n_z)),
        ],
        compiler_params=pltpu.CompilerParams(collective_id=0, has_side_effects=True),
        name="fused",
    )(queries, keys, values, codes, wq_t, wkey_t)


def publish_kernel(*refs):
    half = len(refs) // 2
    for given, out in zip(refs[:half], refs[half:]):
        out[...] = given[...]


def publish(*results):
    return pl.pallas_call(
        publish_kernel,
        out_shape=tuple(jax.ShapeDtypeStruct(r.shape, r.dtype) for r in results),
        in_specs=[pl.BlockSpec(memory_space=VMEM)] * len(results),
        out_specs=(pl.BlockSpec(memory_space=VMEM),) * len(results),
        name="publish",
    )(*results)


def solution(mesh):
    n_seq, n_z = mesh.shape["seq"], mesh.shape["tensor"]

    def shards(queries, keys, values, doc_ids, w_query, w_key):
        count, width = keys.shape
        student, gwq, gwk, kfg = publish(
            *fused(
                queries.reshape(count, width),
                keys,
                values,
                doc_ids.reshape(1, count),
                w_query[0].T,
                w_key.T,
                n_seq,
                n_z,
            )
        )
        return student.reshape(queries.shape), gwq.T[None], gwk.T, kfg.T

    return jax.shard_map(
        shards,
        mesh=mesh,
        in_specs=(
            P("seq", "tensor", None),
            P("seq", None),
            P("seq", None),
            P("seq"),
            P("tensor", None, None),
            P(),
        ),
        out_specs=(P("seq", "tensor", None), P("tensor", None, None), P(), P("seq", "tensor")),
        check_vma=False,
    )
```
